256 devices in a mesh: tm: 32 (over z, y), tok: 8 (over x, core).
Axes of the slice: x: 4, y: 4, z: 8, core: 2. Of those that a mesh axis runs over, the one named last changes fastest.
Arguments:
- states: float32 [128, 2, 256, 1152], P('tm', None, 'tok'), may hold values from -6 to 6
- noise: bfloat16 [128, 2, 256, 1152], P('tm', None, 'tok'), may hold values from -6 to 6
- x_start: float32 [2, 256, 1152], P(None, 'tok'), may hold values from -6 to 6
- timesteps: int32 [128], P('tm'), may hold values from 50 to 999
- step_mod: float32 [128, 3, 1152], P('tm'), may hold values from -40 to 40
- view_mod: float32 [8, 3, 1152], replicated, may hold values from -2 to 2
- view_ids: int32 [128, 2], P('tm'), may hold values from 0 to 7
- w_qkv: bfloat16 [1152, 3456], replicated, may hold values from -0.1875 to 0.1875
- w_out: bfloat16 [1152, 1152], replicated, may hold values from -0.1875 to 0.1875
Outputs:
- new_states: float32 [128, 2, 256, 1152], P('tm', None, 'tok')
The draws below stay inside these ranges and needn't reach their ends.
All inputs are finite; a program needn't handle non-finite values.
Results may differ from the reference program's by a relative error of at most 0.0017.
Values may be sent and summed in bfloat16 or wider, within the bound.
No kernel may reach another device: no remote copies, remote signals or barrier semaphores. Data moves between devices by JAX's collectives and lax.ppermute only.
A program may use at most 128 MiB of HBM per device.

```python
import jax
import jax.numpy as jnp
from jax import lax

D = 1152
HEADS = 16
HEAD_DIM = 72
TOKENS = 256
VIEWS = 2
NVIEW = 8
SWEEPS = 2
WINDOW = 128


def draw_step_mod(key, part):
    shift_key = jax.random.fold_in(key, 11)
    scale_key = jax.random.fold_in(key, 12)
    gate_key = jax.random.fold_in(key, 13)
    shift = 0.5 * jax.random.normal(shift_key, (WINDOW, D), jnp.float32)
    gate = jax.random.normal(gate_key, (WINDOW, D), jnp.float32)
    scale = 0.5 * jax.random.normal(scale_key, (WINDOW, D), jnp.float32)
    return jnp.clip(jnp.stack([shift, scale, gate], axis=1), -40.0, 40.0).astype(jnp.float32)


def set_ends(drawn, key, low, top_value):
    longest = drawn.shape.index(max(drawn.shape))
    spots = []
    for shift in (0, 1):
        where = [jax.random.randint(jax.random.fold_in(key, axis), (), 0, length) for axis, length in enumerate(drawn.shape)]
        where[longest] = (where[longest] + shift) % drawn.shape[longest]
        spots.append(tuple(where))
    return drawn.at[spots[0]].set(low).at[spots[1]].set(top_value)


def block_scale(key, extent, cuts, low, largest):
    level = 1.0
    for dim, blocks in cuts:
        steps = jax.random.uniform(jax.random.fold_in(jax.random.fold_in(key, 6), dim), (blocks,), jnp.float32, low / len(cuts), largest / len(cuts))
        level = level * jnp.repeat(jnp.exp(steps), extent[dim] // blocks).reshape((-1,) + (1,) * (len(extent) - 1 - dim))
    return level


def scatter_about(own_key, extent, width, limit, cuts=(), dtype=jnp.bfloat16):
    array = width * jax.random.normal(own_key, extent, jnp.float32)
    if cuts:
        array = array * block_scale(own_key, extent, cuts, -0.22, 0.18)
    return jnp.clip(array, -limit, limit).astype(dtype)


def setup_inputs(seed: int = 0) -> dict:
    seeds = jax.random.split(jax.random.key(seed), 10)
    states = scatter_about(seeds[0], (WINDOW, VIEWS, TOKENS, D), 1.0, 6.0, ((0, 32), (2, 8)), jnp.float32)
    noise = scatter_about(seeds[1], (WINDOW, VIEWS, TOKENS, D), 1.0, 6.0, ((0, 32), (2, 8)))
    x_start = scatter_about(seeds[2], (VIEWS, TOKENS, D), 1.0, 6.0, ((1, 8),), jnp.float32)
    timesteps = set_ends(jax.random.randint(seeds[3], (WINDOW,), 50, 1000), jax.random.fold_in(seeds[3], 1), 50, 999).astype(jnp.int32)
    step_mod = draw_step_mod(jax.random.fold_in(seeds[9], 71), 0)
    view_mod = scatter_about(seeds[5], (NVIEW, 3, D), 0.3, 2.0, (), jnp.float32)
    view_ids = set_ends(jax.random.randint(seeds[6], (WINDOW, VIEWS), 0, NVIEW), jax.random.fold_in(seeds[6], 1), 0, NVIEW - 1).astype(jnp.int32)
    w_qkv = scatter_about(seeds[7], (D, 3 * D), D ** -0.5, 0.1875)
    w_out = scatter_about(seeds[8], (D, D), D ** -0.5, 0.1875)
    return dict(states=states, noise=noise, x_start=x_start, timesteps=timesteps, step_mod=step_mod, view_mod=view_mod, view_ids=view_ids, w_qkv=w_qkv, w_out=w_out)


def coefficients(steps_index):
    unit = steps_index.astype(jnp.float32) / 1000.0
    beta = 0.1 + 19.9 * unit
    sigma = jnp.sqrt(1.0 - jnp.exp(-(0.1 * unit + 9.95 * unit * unit)))
    coef_state = 0.5 * beta * 0.004
    coef_eps = beta * 0.004 / sigma
    coef_noise = jnp.sqrt(beta * 0.004)
    return (coef_state, coef_eps, coef_noise)

def increment_of(latent, noise_step, step_index, modulation, w_qkv, w_out):
    center = lax.optimization_barrier(jnp.mean(latent, axis=-1, keepdims=True))
    spread = lax.optimization_barrier(jnp.mean((latent - center) ** 2, axis=-1, keepdims=True))
    normed = (latent - center) / jnp.sqrt(spread + 1e-06)
    modulated = (normed * (1.0 + modulation[:, 1][:, None, :]) + modulation[:, 0][:, None, :]).astype(jnp.bfloat16)
    qkv = jnp.dot(modulated.reshape(-1, D), w_qkv, preferred_element_type=jnp.float32).astype(jnp.bfloat16)
    qkv = qkv.reshape(VIEWS, TOKENS, 3, HEADS, HEAD_DIM).astype(jnp.float32)
    queries = qkv[:, :, 0]
    keys = qkv[:, :, 1]
    values = qkv[:, :, 2]
    scores = jnp.einsum('vqhe,vkhe->vhqk', queries, keys) * (1.0 / HEAD_DIM ** 0.5)
    probs = jax.nn.softmax(scores, axis=-1).astype(jnp.bfloat16)
    attended = jnp.einsum('vhqk,vkhe->vqhe', probs.astype(jnp.float32), values).astype(jnp.bfloat16)
    projected = jnp.dot(attended.reshape(-1, D), w_out, preferred_element_type=jnp.float32).reshape(VIEWS, TOKENS, D)
    denoised = latent + modulation[:, 2][:, None, :] * projected
    coef_state, coef_eps, coef_noise = coefficients(step_index)
    return coef_state * latent + coef_eps * denoised + coef_noise * noise_step.astype(jnp.float32)

def reference(states, noise, x_start, timesteps, step_mod, view_mod, view_ids, w_qkv, w_out):
    modulation = step_mod[:, None] + view_mod[view_ids]
    current = states
    for sweep in range(SWEEPS):
        increments = lax.map(lambda items: increment_of(items[0], items[1], items[2], items[3], w_qkv, w_out), (current, noise, timesteps, modulation))
        running = jnp.cumsum(increments, axis=0)
        before = jnp.concatenate([jnp.zeros_like(running[:1]), running[:-1]], axis=0)
        current = x_start[None] + before
    return current
```

```python
import jax
import jax.numpy as jnp
from jax import lax
from jax.experimental import pallas as pl
from jax.experimental.pallas import tpu as pltpu
from jax.sharding import Mesh
from jax.sharding import PartitionSpec as P

HEADS = 16
SWEEPS = 2
LANES = 128
VMEM = pl.BlockSpec(memory_space=pltpu.VMEM)
SMEM = pl.BlockSpec(memory_space=pltpu.SMEM)


def shifted(value, axis, shift):
    size = lax.axis_size(axis)
    return lax.ppermute(value, axis, [(i, (i + shift) % size) for i in range(size)])


def from_below(value, axis, shift):
    size = lax.axis_size(axis)
    return lax.ppermute(value, axis, [(i, i + shift) for i in range(size - shift)])


def call(body, outs, specs, *args, scratch=()):
    return pl.pallas_call(
        body,
        out_shape=outs,
        in_specs=specs,
        out_specs=jax.tree.map(lambda _: VMEM, outs),
        scratch_shapes=list(scratch),
        compiler_params=pltpu.CompilerParams(vmem_limit_bytes=48 * 2**20),
    )(*args)


def normed_rows(rows, shift, scale):
    center = jnp.mean(rows, axis=-1, keepdims=True)
    off = rows - center
    spread = jnp.mean(off * off, axis=-1, keepdims=True)
    normed = off / jnp.sqrt(spread + 1e-06)
    return (normed * (1.0 + scale) + shift).astype(jnp.bfloat16)


def modulation_row(where_ref, step_ref, view_ref, step, part):
    return step_ref[step, part : part + 1, :] + view_ref[where_ref[2 + step], part : part + 1, :]


def enter_body(where_ref, mine_ref, peer_ref, step_ref, view_ref, x_ref, *mod_refs):
    place = where_ref[0]
    steps = mine_ref.shape[0]
    for r in range(steps):
        step = lax.rem(place + r, steps)
        shift = modulation_row(where_ref, step_ref, view_ref, step, 0)
        scale = modulation_row(where_ref, step_ref, view_ref, step, 1)
        rows = jnp.concatenate([mine_ref[step], peer_ref[step]], axis=0)
        x_ref[step] = rows
        mod_refs[r][...] = normed_rows(rows, shift, scale)


def resume_body(where_ref, start_ref, before_ref, l0, l1, l2, l3, step_ref, view_ref, x_ref, *rest):
    mod_refs, base_ref = rest[:-1], rest[-1]
    place, spot = where_ref[0], where_ref[1]
    steps = before_ref.shape[0]
    lower = (l0, l1, l2, l3)
    part = l0.shape[0]
    for r in range(len(lower)):
        rows = pl.ds(pl.multiple_of(lax.rem(spot + len(lower) - r, len(lower)) * part, part), part)
        base_ref[rows, :] = lower[r][...]
    for r in range(steps):
        step = lax.rem(place + r, steps)
        rows = start_ref[...] + (base_ref[...] + before_ref[step])
        x_ref[step] = rows
        if mod_refs:
            shift = modulation_row(where_ref, step_ref, view_ref, step, 0)
            scale = modulation_row(where_ref, step_ref, view_ref, step, 1)
            mod_refs[r][...] = normed_rows(rows, shift, scale)


def attend_body(a0, a1, a2, a3, w_ref, mask_ref, o0, o1, o2, o3, rows_ref, qkv_ref):
    pieces = (a0, a1, a2, a3)
    part, width = a0.shape
    for r in range(4):
        rows_ref[r * part : (r + 1) * part, :] = pieces[r][...]
    qkv_ref[...] = jnp.dot(
        rows_ref[...], w_ref[...], preferred_element_type=jnp.float32
    ).astype(jnp.bfloat16)
    size = width // HEADS
    tiles = [None] * (width // LANES)
    for h in range(HEADS):
        first = h * size // LANES
        last = ((h + 1) * size - 1) // LANES
        low, high = first * LANES, (last + 1) * LANES
        q = qkv_ref[:, low:high] * mask_ref[h : h + 1, low:high]
        k = qkv_ref[:, width + low : width + high]
        v = qkv_ref[:, 2 * width + low : 2 * width + high]
        scores = lax.dot_general(
            q, k, (((1,), (1,)), ((), ())), preferred_element_type=jnp.float32
        ) * (1.0 / size**0.5)
        top = jnp.max(scores, axis=-1, keepdims=True)
        powers = jnp.exp(scores - top)
        probs = (powers / jnp.sum(powers, axis=-1, keepdims=True)).astype(jnp.bfloat16)
        out = jnp.dot(probs, v, preferred_element_type=jnp.float32)
        for t in range(first, last + 1):
            piece = out[:, t * LANES - low : (t + 1) * LANES - low]
            if tiles[t] is not None:
                lane = lax.broadcasted_iota(jnp.int32, piece.shape, 1) + t * LANES
                piece = jnp.where(lane >= h * size, piece, tiles[t])
            tiles[t] = piece
    outs = (o0, o1, o2, o3)
    for t, tile in enumerate(tiles):
        tile = tile.astype(jnp.bfloat16)
        for r in range(4):
            outs[r][:, t * LANES : (t + 1) * LANES] = tile[r * part : (r + 1) * part]


def project_body(
    where_ref, coef_ref, a0, a1, a2, a3, w_ref, x_ref, mine_ref, peer_ref, step_ref, view_ref, before_ref, *rest
):
    total_refs, rows_ref, proj_ref, total_ref = rest[:-3], rest[-3], rest[-2], rest[-1]
    place, spot = where_ref[0], where_ref[1]
    pieces = (a0, a1, a2, a3)
    part = a0.shape[0]
    steps = len(pieces)
    for r in range(steps):
        rows = pl.ds(pl.multiple_of(lax.rem(place + r, steps) * part, part), part)
        rows_ref[rows, :] = pieces[r][...]
    proj_ref[...] = jnp.dot(rows_ref[...], w_ref[...], preferred_element_type=jnp.float32)
    running = None
    for step in range(steps):
        gate = modulation_row(where_ref, step_ref, view_ref, step, 2)
        rows = x_ref[step]
        denoised = rows + gate * proj_ref[step * part : (step + 1) * part, :]
        drawn = jnp.concatenate([mine_ref[step], peer_ref[step]], axis=0).astype(jnp.float32)
        increment = coef_ref[0, step] * rows + coef_ref[1, step] * denoised + coef_ref[2, step] * drawn
        before_ref[step] = jnp.zeros_like(increment) if running is None else running
        running = increment if running is None else running + increment
    total_ref[...] = running
    share = total_refs[0].shape[0]
    for r in range(len(total_refs)):
        rows = pl.ds(pl.multiple_of(lax.rem(spot + r, len(total_refs)) * share, share), share)
        total_refs[r][...] = total_ref[rows, :]


def coefficients(steps_index):
    unit = steps_index.astype(jnp.float32) / 1000.0
    beta = 0.1 + 19.9 * unit
    sigma = jnp.sqrt(1.0 - jnp.exp(-(0.1 * unit + 9.95 * unit * unit)))
    coef_state = 0.5 * beta * 0.004
    coef_eps = beta * 0.004 / sigma
    coef_noise = jnp.sqrt(beta * 0.004)
    return (coef_state, coef_eps, coef_noise)


def earlier_sum(totals):
    spot = lax.axis_index("y")
    peers = lax.axis_size("y")
    mine = [totals[0]] + [shifted(totals[r], "y", r) for r in range(1, peers)]
    held = []
    for p in range(peers):
        r = lax.rem(spot - p + peers, peers)
        value = mine[0]
        for k in range(1, peers):
            value = jnp.where(r == k, mine[k], value)
        held.append(value)
    inside = [jnp.zeros_like(held[0])]
    for p in range(peers):
        inside.append(inside[-1] + held[p])
    running = inside.pop()
    below = jnp.zeros_like(running)
    shift = 1
    while shift < lax.axis_size("z"):
        passed = from_below(running, "z", shift)
        below = below + passed
        running = running + passed
        shift *= 2
    lower = []
    for r in range(peers):
        p = lax.rem(spot + r, peers)
        value = inside[0]
        for k in range(1, peers):
            value = jnp.where(p == k, inside[k], value)
        lower.append(value + below)
    return [lower[0]] + [shifted(lower[r], "y", r) for r in range(1, peers)]


def per_device(states, noise, x_start, timesteps, step_mod, view_mod, view_ids, w_qkv, w_out):
    steps, views, part, width = states.shape
    place, spot, core = (lax.axis_index(a) for a in ("x", "y", "c"))
    other = 1 - core
    f32, bf16 = jnp.float32, jnp.bfloat16
    rows = 2 * part

    def own(a, axis):
        return lax.dynamic_index_in_dim(a, core, axis, keepdims=False)

    def from_peer(a, axis):
        return shifted(lax.dynamic_index_in_dim(a, other, axis, keepdims=False), "c", 1)

    where = jnp.concatenate([jnp.stack([place, spot]).astype(jnp.int32), own(view_ids, 1)])
    coefs = jnp.stack(coefficients(timesteps))
    start = jnp.concatenate([own(x_start, 0), from_peer(x_start, 0)], axis=0)
    noise_mine, noise_peer = own(noise, 1), from_peer(noise, 1)
    size = width // HEADS
    column = jnp.arange(width, dtype=jnp.int32)[None, :]
    head = jnp.arange(HEADS, dtype=jnp.int32)[:, None]
    mask = ((column >= head * size) & (column < (head + 1) * size)).astype(bf16)

    x_shape = jax.ShapeDtypeStruct((steps, rows, width), f32)
    piece = jax.ShapeDtypeStruct((rows, width), bf16)
    share = jax.ShapeDtypeStruct((rows // lax.axis_size("y"), width), f32)
    x, *mods = call(
        enter_body,
        [x_shape] + [piece] * steps,
        [SMEM] + [VMEM] * 4,
        where,
        own(states, 1),
        from_peer(states, 1),
        step_mod,
        view_mod,
    )
    for sweep in range(SWEEPS):
        arrived = [mods[0]] + [shifted(mods[r], "x", r) for r in range(1, steps)]
        attended = call(
            attend_body,
            [piece] * steps,
            [VMEM] * 6,
            *arrived,
            w_qkv,
            mask,
            scratch=[pltpu.VMEM((steps * rows, width), bf16), pltpu.VMEM((steps * rows, 3 * width), bf16)],
        )
        back = [attended[0]] + [shifted(attended[r], "x", -r) for r in range(1, steps)]
        before, *totals = call(
            project_body,
            [x_shape] + [share] * lax.axis_size("y"),
            [SMEM] * 2 + [VMEM] * 10,
            where,
            coefs,
            *back,
            w_out,
            x,
            noise_mine,
            noise_peer,
            step_mod,
            view_mod,
            scratch=[
                pltpu.VMEM((steps * rows, width), bf16),
                pltpu.VMEM((steps * rows, width), f32),
                pltpu.VMEM((rows, width), f32),
            ],
        )
        lower = earlier_sum(totals)
        more = sweep + 1 < SWEEPS
        x, *mods = call(
            resume_body,
            [x_shape] + ([piece] * steps if more else []),
            [SMEM] + [VMEM] * 8,
            where,
            start,
            before,
            *lower,
            step_mod,
            view_mod,
            scratch=[pltpu.VMEM((rows, width), f32)],
        )
    mine, given = x[:, :part], shifted(x[:, part:], "c", 1)
    low = jnp.where(core == 0, mine, given)
    high = jnp.where(core == 0, given, mine)
    return jnp.stack([low, high], axis=1)


def solution(mesh):
    finer = Mesh(mesh.devices.reshape(8, 4, 4, 2), ("z", "y", "x", "c"))
    tm, tok = ("z", "y"), ("x", "c")
    placed = (
        P(tm, None, tok, None),
        P(tm, None, tok, None),
        P(None, tok, None),
        P(tm),
        P(tm, None, None),
        P(),
        P(tm, None),
        P(),
        P(),
    )
    return jax.shard_map(
        per_device, mesh=finer, in_specs=placed, out_specs=P(tm, None, tok, None), check_vma=False
    )
```

```python
import jax
import jax.numpy as jnp
from jax import lax
from jax.experimental import pallas as pl
from jax.experimental.pallas import tpu as pltpu
from jax.sharding import Mesh
from jax.sharding import PartitionSpec as P

HEADS = 16
SWEEPS = 2
LANES = 128
BLOCKS = 4
LOG2E = 1.4426950408889634
HALF = ("v", "u", "y")
PLANES = ("w", "v", "u")
VMEM = pl.BlockSpec(memory_space=pltpu.VMEM)
SMEM = pl.BlockSpec(memory_space=pltpu.SMEM)


def shifted(value, axis, shift):
    size = lax.axis_size(axis)
    return lax.ppermute(value, axis, [(i, (i + shift) % size) for i in range(size)])


def call(body, outs, specs, *args, scratch=()):
    return pl.pallas_call(
        body,
        out_shape=outs,
        in_specs=specs,
        out_specs=jax.tree.map(lambda _: VMEM, outs),
        scratch_shapes=list(scratch),
        compiler_params=pltpu.CompilerParams(vmem_limit_bytes=48 * 2**20),
    )(*args)


def normed_rows(rows, shift, scale):
    center = jnp.mean(rows, axis=-1, keepdims=True)
    off = rows - center
    spread = jnp.mean(off * off, axis=-1, keepdims=True)
    normed = off / jnp.sqrt(spread + 1e-06)
    return (normed * (1.0 + scale) + shift).astype(jnp.bfloat16)


def modulation_row(where_ref, step_ref, view_ref, step, part):
    return step_ref[step, part : part + 1, :] + view_ref[where_ref[2 + step], part : part + 1, :]


def enter_body(where_ref, mine_ref, peer_ref, step_ref, view_ref, x_ref, *mod_refs):
    place = where_ref[0]
    steps = mine_ref.shape[0]
    for r in range(steps):
        step = lax.rem(place + r, steps)
        shift = modulation_row(where_ref, step_ref, view_ref, step, 0)
        scale = modulation_row(where_ref, step_ref, view_ref, step, 1)
        rows = jnp.concatenate([mine_ref[step], peer_ref[step]], axis=0)
        x_ref[step] = rows
        mod_refs[r][...] = normed_rows(rows, shift, scale)


def block_rows(flip, block, blocks, part):
    place = block + flip * (blocks - 1 - 2 * block)
    return pl.ds(pl.multiple_of(place * part, part), part)


def resume_body(where_ref, start_ref, before_ref, lower_ref, step_ref, view_ref, x_ref, *rest):
    mod_refs, base_ref = rest[:-1], rest[-1]
    place, flip = where_ref[0], where_ref[1]
    steps = before_ref.shape[0]
    part = lower_ref.shape[0] // BLOCKS
    for block in range(BLOCKS):
        base_ref[block * part : (block + 1) * part, :] = lower_ref[block_rows(flip, block, BLOCKS, part), :]
    for r in range(steps):
        step = lax.rem(place + r, steps)
        rows = start_ref[...] + (base_ref[...] + before_ref[step])
        x_ref[step] = rows
        if mod_refs:
            shift = modulation_row(where_ref, step_ref, view_ref, step, 0)
            scale = modulation_row(where_ref, step_ref, view_ref, step, 1)
            mod_refs[r][...] = normed_rows(rows, shift, scale)


def attend_body(a0, a1, a2, a3, w_ref, mask_ref, o0, o1, o2, o3, rows_ref, qkv_ref):
    pieces = (a0, a1, a2, a3)
    part, width = a0.shape
    for r in range(4):
        rows_ref[r * part : (r + 1) * part, :] = pieces[r][...]
    qkv_ref[...] = jnp.dot(
        rows_ref[...], w_ref[...], preferred_element_type=jnp.float32
    ).astype(jnp.bfloat16)
    size = width // HEADS
    tiles = [None] * (width // LANES)
    for h in range(HEADS):
        first = h * size // LANES
        last = ((h + 1) * size - 1) // LANES
        low, high = first * LANES, (last + 1) * LANES
        q = qkv_ref[:, low:high] * mask_ref[h : h + 1, low:high]
        k = qkv_ref[:, width + low : width + high]
        v = qkv_ref[:, 2 * width + low : 2 * width + high]
        scores = lax.dot_general(q, k, (((1,), (1,)), ((), ())), preferred_element_type=jnp.float32)
        top = jnp.max(scores, axis=-1, keepdims=True)
        powers = jnp.exp2((scores - top) * (LOG2E / size**0.5))
        share = 1.0 / jnp.sum(powers, axis=-1, keepdims=True)
        out = jnp.dot(powers.astype(jnp.bfloat16), v, preferred_element_type=jnp.float32) * share
        for t in range(first, last + 1):
            piece = out[:, t * LANES - low : (t + 1) * LANES - low]
            if tiles[t] is not None:
                lane = lax.broadcasted_iota(jnp.int32, piece.shape, 1) + t * LANES
                piece = jnp.where(lane >= h * size, piece, tiles[t])
            tiles[t] = piece
    outs = (o0, o1, o2, o3)
    for t, tile in enumerate(tiles):
        tile = tile.astype(jnp.bfloat16)
        for r in range(4):
            outs[r][:, t * LANES : (t + 1) * LANES] = tile[r * part : (r + 1) * part]


def project_body(
    where_ref,
    coef_ref,
    a0,
    a1,
    a2,
    a3,
    w_ref,
    x_ref,
    mine_ref,
    peer_ref,
    step_ref,
    view_ref,
    before_ref,
    total_ref,
    rows_ref,
    proj_ref,
):
    place, flip = where_ref[0], where_ref[1]
    pieces = (a0, a1, a2, a3)
    part = a0.shape[0]
    steps = len(pieces)
    for r in range(steps):
        rows = pl.ds(pl.multiple_of(lax.rem(place + r, steps) * part, part), part)
        rows_ref[rows, :] = pieces[r][...]
    proj_ref[...] = jnp.dot(rows_ref[...], w_ref[...], preferred_element_type=jnp.float32)
    running = None
    for step in range(steps):
        gate = modulation_row(where_ref, step_ref, view_ref, step, 2)
        rows = x_ref[step]
        denoised = rows + gate * proj_ref[step * part : (step + 1) * part, :]
        drawn = jnp.concatenate([mine_ref[step], peer_ref[step]], axis=0).astype(jnp.float32)
        increment = coef_ref[0, step] * rows + coef_ref[1, step] * denoised + coef_ref[2, step] * drawn
        before_ref[step] = jnp.zeros_like(increment) if running is None else running
        running = increment if running is None else running + increment
    share = part // BLOCKS
    for block in range(BLOCKS):
        total_ref[block_rows(flip, block, BLOCKS, share), :] = running[block * share : (block + 1) * share]


def coefficients(steps_index):
    unit = steps_index.astype(jnp.float32) / 1000.0
    beta = 0.1 + 19.9 * unit
    sigma = jnp.sqrt(1.0 - jnp.exp(-(0.1 * unit + 9.95 * unit * unit)))
    coef_state = 0.5 * beta * 0.004
    coef_eps = beta * 0.004 / sigma
    coef_noise = jnp.sqrt(beta * 0.004)
    return (coef_state, coef_eps, coef_noise)


def inside_body(held_ref, before_ref, all_ref):
    running = jnp.zeros(held_ref.shape[1:], held_ref.dtype)
    for q in range(held_ref.shape[0]):
        before_ref[q] = running
        running = running + held_ref[q]
    all_ref[...] = running


def earlier_sum(total):
    places = lax.axis_size(HALF)
    rows, width = total.shape
    shares = total.reshape(places, rows // places, width)
    held = lax.all_to_all(shares, HALF, 0, 0, tiled=True)
    before, whole = call(
        inside_body,
        [jax.ShapeDtypeStruct(shares.shape, total.dtype), jax.ShapeDtypeStruct(shares.shape[1:], total.dtype)],
        [VMEM],
        held,
    )
    planes = lax.axis_size(PLANES)
    below = lax.ppermute(whole, PLANES, [(i, planes - 1 - i) for i in range(planes)])
    below = jnp.where(lax.axis_index("w") == 1, below, jnp.zeros_like(below))
    lower = lax.all_to_all(before + below[None], HALF, 0, 0, tiled=True)
    return lower.reshape(rows, width)


def per_device(states, noise, x_start, timesteps, step_mod, view_mod, view_ids, w_qkv, w_out):
    steps, views, part, width = states.shape
    place, flip, core = (lax.axis_index(a) for a in ("x", "w", "c"))
    other = 1 - core
    f32, bf16 = jnp.float32, jnp.bfloat16
    rows = 2 * part

    def own(a, axis):
        return lax.dynamic_index_in_dim(a, core, axis, keepdims=False)

    def from_peer(a, axis):
        return shifted(lax.dynamic_index_in_dim(a, other, axis, keepdims=False), "c", 1)

    where = jnp.concatenate([jnp.stack([place, flip]).astype(jnp.int32), own(view_ids, 1)])
    coefs = jnp.stack(coefficients(timesteps))
    start = jnp.concatenate([own(x_start, 0), from_peer(x_start, 0)], axis=0)
    noise_mine, noise_peer = own(noise, 1), from_peer(noise, 1)
    size = width // HEADS
    column = jnp.arange(width, dtype=jnp.int32)[None, :]
    head = jnp.arange(HEADS, dtype=jnp.int32)[:, None]
    mask = ((column >= head * size) & (column < (head + 1) * size)).astype(bf16)

    x_shape = jax.ShapeDtypeStruct((steps, rows, width), f32)
    piece = jax.ShapeDtypeStruct((rows, width), bf16)
    total_shape = jax.ShapeDtypeStruct((rows, width), f32)
    x, *mods = call(
        enter_body,
        [x_shape] + [piece] * steps,
        [SMEM] + [VMEM] * 4,
        where,
        own(states, 1),
        from_peer(states, 1),
        step_mod,
        view_mod,
    )
    for sweep in range(SWEEPS):
        arrived = [mods[0]] + [shifted(mods[r], "x", r) for r in range(1, steps)]
        attended = call(
            attend_body,
            [piece] * steps,
            [VMEM] * 6,
            *arrived,
            w_qkv,
            mask,
            scratch=[pltpu.VMEM((steps * rows, width), bf16), pltpu.VMEM((steps * rows, 3 * width), bf16)],
        )
        back = [attended[0]] + [shifted(attended[r], "x", -r) for r in range(1, steps)]
        before, total = call(
            project_body,
            [x_shape, total_shape],
            [SMEM] * 2 + [VMEM] * 10,
            where,
            coefs,
            *back,
            w_out,
            x,
            noise_mine,
            noise_peer,
            step_mod,
            view_mod,
            scratch=[
                pltpu.VMEM((steps * rows, width), bf16),
                pltpu.VMEM((steps * rows, width), f32),
            ],
        )
        lower = earlier_sum(total)
        more = sweep + 1 < SWEEPS
        x, *mods = call(
            resume_body,
            [x_shape] + ([piece] * steps if more else []),
            [SMEM] + [VMEM] * 5,
            where,
            start,
            before,
            lower,
            step_mod,
            view_mod,
            scratch=[pltpu.VMEM((rows, width), f32)],
        )
    mine, given = x[:, :part], shifted(x[:, part:], "c", 1)
    low = jnp.where(core == 0, mine, given)
    high = jnp.where(core == 0, given, mine)
    return jnp.stack([low, high], axis=1)


def solution(mesh):
    finer = Mesh(mesh.devices.reshape(2, 2, 2, 4, 4, 2), ("w", "v", "u", "y", "x", "c"))
    tm, tok = ("w", "v", "u", "y"), ("x", "c")
    placed = (
        P(tm, None, tok, None),
        P(tm, None, tok, None),
        P(None, tok, None),
        P(tm),
        P(tm, None, None),
        P(),
        P(tm, None),
        P(),
        P(),
    )
    return jax.shard_map(
        per_device, mesh=finer, in_specs=placed, out_specs=P(tm, None, tok, None), check_vma=False
    )
```

```python
import jax
import jax.numpy as jnp
from jax import lax
from jax.experimental import pallas as pl
from jax.experimental.pallas import tpu as pltpu
from jax.sharding import Mesh
from jax.sharding import PartitionSpec as P

HEADS = 16
SWEEPS = 2
LANES = 128
BLOCKS = 4
LOG2E = 1.4426950408889634
HALF = ("v", "u", "y")
PLANES = ("w", "v", "u")
VMEM = pl.BlockSpec(memory_space=pltpu.VMEM)
SMEM = pl.BlockSpec(memory_space=pltpu.SMEM)


def shifted(value, axis, shift):
    size = lax.axis_size(axis)
    return lax.ppermute(value, axis, [(i, (i + shift) % size) for i in range(size)])


def call(body, outs, specs, *args, scratch=()):
    return pl.pallas_call(
        body,
        out_shape=outs,
        in_specs=specs,
        out_specs=jax.tree.map(lambda _: VMEM, outs),
        scratch_shapes=list(scratch),
        compiler_params=pltpu.CompilerParams(vmem_limit_bytes=16 * 2**20),
    )(*args)


def normed_rows(rows, shift, scale):
    center = jnp.mean(rows, axis=-1, keepdims=True)
    off = rows - center
    spread = jnp.mean(off * off, axis=-1, keepdims=True)
    normed = off / jnp.sqrt(spread + 1e-06)
    return (normed * (1.0 + scale) + shift).astype(jnp.bfloat16)


def modulation_row(where_ref, step_ref, view_ref, step, part):
    return step_ref[step, part : part + 1, :] + view_ref[where_ref[3 + step], part : part + 1, :]


def enter_body(where_ref, mine_ref, start_mine, peer_ref, step_ref, view_ref, x_ref, start_ref, *mod_refs):
    place = where_ref[0]
    start_ref[...] = jnp.concatenate([start_mine[...], peer_ref[mine_ref.shape[0]]], axis=0)
    steps = mine_ref.shape[0]
    for r in range(steps):
        step = lax.rem(place + r, steps)
        shift = modulation_row(where_ref, step_ref, view_ref, step, 0)
        scale = modulation_row(where_ref, step_ref, view_ref, step, 1)
        rows = jnp.concatenate([mine_ref[step], peer_ref[step]], axis=0)
        x_ref[step] = rows
        mod_refs[r][...] = normed_rows(rows, shift, scale)


def block_rows(flip, block, blocks, part):
    place = block + flip * (blocks - 1 - 2 * block)
    return pl.ds(pl.multiple_of(place * part, part), part)


def resume_body(
    where_ref, start_ref, mine_before, peer_before, lower_ref, step_ref, view_ref, x_ref, *rest
):
    mod_refs, base_ref = rest[:-1], rest[-1]
    place, flip = where_ref[0], where_ref[1]
    steps = mine_before.shape[0]
    part = lower_ref.shape[0] // BLOCKS
    for block in range(BLOCKS):
        base_ref[block * part : (block + 1) * part, :] = lower_ref[block_rows(flip, block, BLOCKS, part), :]
    for r in range(steps):
        step = lax.rem(place + r, steps)
        before = jnp.concatenate([mine_before[step], peer_before[step]], axis=0)
        rows = start_ref[...] + (base_ref[...] + before)
        x_ref[step] = rows
        shift = modulation_row(where_ref, step_ref, view_ref, step, 0)
        scale = modulation_row(where_ref, step_ref, view_ref, step, 1)
        mod_refs[r][...] = normed_rows(rows, shift, scale)


def finish_body(where_ref, start_ref, mine_before, peer_before, mine_lower, peer_lower, out_ref):
    flip, core = where_ref[1], where_ref[2]
    blocks = BLOCKS // 2
    part = mine_lower.shape[0] // blocks
    for view, before_ref, lower_ref in ((core, mine_before, mine_lower), (1 - core, peer_before, peer_lower)):
        for block in range(blocks):
            rows = slice(block * part, (block + 1) * part)
            base = lower_ref[block_rows(flip, block, blocks, part), :]
            for step in range(before_ref.shape[0]):
                out_ref[step, view, rows, :] = start_ref[view, rows, :] + (base + before_ref[step, rows, :])


def project_rows(rows, w_ref):
    return jnp.dot(rows, w_ref[...], preferred_element_type=jnp.float32).astype(jnp.bfloat16)


def first_body(a0, w_ref, qkv_ref):
    qkv_ref[...] = project_rows(a0[...], w_ref)


def attend(q_ref, kv_ref, mask_ref, outs):
    width = mask_ref.shape[1]
    part = outs[0].shape[0]
    size = width // HEADS
    tiles = [None] * (width // LANES)
    for h in range(HEADS):
        first = h * size // LANES
        last = ((h + 1) * size - 1) // LANES
        low, high = first * LANES, (last + 1) * LANES
        q = q_ref[:, low:high] * mask_ref[h : h + 1, low:high]
        k = kv_ref[:, width + low : width + high]
        v = kv_ref[:, 2 * width + low : 2 * width + high]
        scores = lax.dot_general(q, k, (((1,), (1,)), ((), ())), preferred_element_type=jnp.float32)
        top = jnp.max(scores, axis=-1, keepdims=True)
        powers = jnp.exp2((scores - top) * (LOG2E / size**0.5))
        share = 1.0 / jnp.sum(powers, axis=-1, keepdims=True)
        out = jnp.dot(powers.astype(jnp.bfloat16), v, preferred_element_type=jnp.float32) * share
        for t in range(first, last + 1):
            piece = out[:, t * LANES - low : (t + 1) * LANES - low]
            if tiles[t] is not None:
                lane = lax.broadcasted_iota(jnp.int32, piece.shape, 1) + t * LANES
                piece = jnp.where(lane >= h * size, piece, tiles[t])
            tiles[t] = piece
    for t, tile in enumerate(tiles):
        tile = tile.astype(jnp.bfloat16)
        for r, out in enumerate(outs):
            out[:, t * LANES : (t + 1) * LANES] = tile[r * part : (r + 1) * part]


def others_body(first_ref, a1, a2, a3, w_ref, mask_ref, o1, o2, o3, qkv_ref, rows_ref):
    part = a1.shape[0]
    for r, piece in enumerate((a1, a2, a3)):
        rows_ref[r * part : (r + 1) * part, :] = piece[...]
    qkv_ref[: 3 * part, :] = project_rows(rows_ref[...], w_ref)
    qkv_ref[3 * part :, :] = first_ref[...]
    attend(qkv_ref.at[: 3 * part], qkv_ref, mask_ref, (o1, o2, o3))


def own_body(first_ref, qkv_ref, mask_ref, o0):
    attend(first_ref, qkv_ref, mask_ref, (o0,))


def base_body(coef_ref, x_ref, mine_ref, peer_ref, base_ref):
    for step in range(x_ref.shape[0]):
        rows = x_ref[step]
        drawn = jnp.concatenate([mine_ref[step], peer_ref[step]], axis=0).astype(jnp.float32)
        base_ref[step] = (coef_ref[0, step] + coef_ref[1, step]) * rows + coef_ref[2, step] * drawn


def project_body(
    where_ref,
    coef_ref,
    a0,
    a1,
    a2,
    a3,
    w_ref,
    base_ref,
    step_ref,
    view_ref,
    mine_before,
    peer_before,
    total_ref,
    rows_ref,
    proj_ref,
):
    place, flip = where_ref[0], where_ref[1]
    pieces = (a0, a1, a2, a3)
    part = a0.shape[0]
    half = part // 2
    steps = len(pieces)
    for r in range(steps):
        rows = pl.ds(pl.multiple_of(lax.rem(place + r, steps) * part, part), part)
        rows_ref[rows, :] = pieces[r][...]
    proj_ref[...] = jnp.dot(rows_ref[...], w_ref[...], preferred_element_type=jnp.float32)
    running = jnp.zeros((part, proj_ref.shape[1]), jnp.float32)
    for step in range(steps):
        gate = modulation_row(where_ref, step_ref, view_ref, step, 2) * coef_ref[1, step]
        mine_before[step] = running[:half]
        peer_before[step] = running[half:]
        running = running + (base_ref[step] + gate * proj_ref[step * part : (step + 1) * part, :])
    share = part // BLOCKS
    for block in range(BLOCKS):
        total_ref[block_rows(flip, block, BLOCKS, share), :] = running[block * share : (block + 1) * share]


def coefficients(steps_index):
    unit = steps_index.astype(jnp.float32) / 1000.0
    beta = 0.1 + 19.9 * unit
    sigma = jnp.sqrt(1.0 - jnp.exp(-(0.1 * unit + 9.95 * unit * unit)))
    coef_state = 0.5 * beta * 0.004
    coef_eps = beta * 0.004 / sigma
    coef_noise = jnp.sqrt(beta * 0.004)
    return (coef_state, coef_eps, coef_noise)


def inside_body(held_ref, before_ref, all_ref):
    running = jnp.zeros(held_ref.shape[1:], held_ref.dtype)
    for q in range(held_ref.shape[0]):
        before_ref[q] = running
        running = running + held_ref[q]
    all_ref[...] = running


def earlier_sum(total, beside=None):
    places = lax.axis_size(HALF)
    rows, width = total.shape
    shares = total.reshape(places, rows // places, width)
    held = lax.all_to_all(shares, HALF, 0, 0, tiled=True)
    before, whole = call(
        inside_body,
        [jax.ShapeDtypeStruct(shares.shape, total.dtype), jax.ShapeDtypeStruct(shares.shape[1:], total.dtype)],
        [VMEM],
        held,
    )
    planes = lax.axis_size(PLANES)
    below = lax.ppermute(whole, PLANES, [(i, planes - 1 - i) for i in range(planes)])
    if beside is not None:
        below, beside = lax.optimization_barrier((below, shifted(beside, "c", 1)))
    below = jnp.where(lax.axis_index("w") == 1, below, jnp.zeros_like(below))
    lower = lax.all_to_all(before + below[None], HALF, 0, 0, tiled=True)
    return lower, beside


def per_device(states, noise, x_start, timesteps, step_mod, view_mod, view_ids, w_qkv, w_out):
    steps, views, part, width = states.shape
    place, flip, core = (lax.axis_index(a) for a in ("x", "w", "c"))
    other = 1 - core
    f32, bf16 = jnp.float32, jnp.bfloat16
    rows = 2 * part

    def own(a, axis):
        return lax.dynamic_index_in_dim(a, core, axis, keepdims=False)

    def given(a, axis):
        return lax.dynamic_index_in_dim(a, other, axis, keepdims=False)

    def shape(*dims, kind=f32):
        return jax.ShapeDtypeStruct(dims, kind)

    swapped = shifted(jnp.concatenate([given(states, 1), given(x_start, 0)[None]], axis=0), "c", 1)
    states_mine, start_mine = own(states, 1), own(x_start, 0)
    noise_mine, noise_peer = own(noise, 1), shifted(given(noise, 1), "c", 1)
    where = jnp.concatenate([jnp.stack([place, flip, core]).astype(jnp.int32), own(view_ids, 1)])
    coefs = jnp.stack(coefficients(timesteps))
    size = width // HEADS
    column = jnp.arange(width, dtype=jnp.int32)[None, :]
    head = jnp.arange(HEADS, dtype=jnp.int32)[:, None]
    mask = ((column >= head * size) & (column < (head + 1) * size)).astype(bf16)

    x_shape = shape(steps, rows, width)
    half = shape(steps, part, width)
    piece = shape(rows, width, kind=bf16)
    x, start, *mods = call(
        enter_body,
        [x_shape, shape(rows, width)] + [piece] * steps,
        [SMEM] + [VMEM] * 5,
        where,
        states_mine,
        start_mine,
        swapped,
        step_mod,
        view_mod,
    )
    for sweep in range(SWEEPS):
        arrived = [shifted(mods[r], "x", r) for r in range(1, steps)]
        first = call(first_body, shape(rows, 3 * width, kind=bf16), [VMEM] * 2, mods[0], w_qkv)
        *attended, qkv = call(
            others_body,
            [piece] * (steps - 1) + [shape(steps * rows, 3 * width, kind=bf16)],
            [VMEM] * 6,
            first,
            *arrived,
            w_qkv,
            mask,
            scratch=[pltpu.VMEM(((steps - 1) * rows, width), bf16)],
        )
        back = [shifted(attended[r - 1], "x", -r) for r in range(1, steps)]
        kept = call(own_body, piece, [VMEM] * 3, first, qkv, mask)
        base = call(base_body, x_shape, [SMEM] + [VMEM] * 3, coefs, x, noise_mine, noise_peer)
        mine_before, peer_before, total = call(
            project_body,
            [half, half, shape(rows, width)],
            [SMEM] * 2 + [VMEM] * 8,
            where,
            coefs,
            kept,
            *back,
            w_out,
            base,
            step_mod,
            view_mod,
            scratch=[pltpu.VMEM((steps * rows, width), bf16), pltpu.VMEM((steps * rows, width), f32)],
        )
        if sweep + 1 == SWEEPS:
            break
        lower, _ = earlier_sum(total)
        x, *mods = call(
            resume_body,
            [x_shape] + [piece] * steps,
            [SMEM] + [VMEM] * 6,
            where,
            start,
            mine_before,
            peer_before,
            lower.reshape(rows, width),
            step_mod,
            view_mod,
            scratch=[pltpu.VMEM((rows, width), f32)],
        )
    lower, peer_before = earlier_sum(total, peer_before)
    places = lower.shape[0] // 2
    lower_mine = lax.dynamic_slice_in_dim(lower, flip * places, places)
    lower_peer = shifted(lax.dynamic_slice_in_dim(lower, (1 - flip) * places, places), "c", 1)
    return call(
        finish_body,
        shape(*states.shape),
        [SMEM] + [VMEM] * 5,
        where,
        x_start,
        mine_before,
        peer_before,
        lower_mine.reshape(part, width),
        lower_peer.reshape(part, width),
    )


def solution(mesh):
    finer = Mesh(mesh.devices.reshape(2, 2, 2, 4, 4, 2), ("w", "v", "u", "y", "x", "c"))
    tm, tok = ("w", "v", "u", "y"), ("x", "c")
    placed = (
        P(tm, None, tok, None),
        P(tm, None, tok, None),
        P(None, tok, None),
        P(tm),
        P(tm, None, None),
        P(),
        P(tm, None),
        P(),
        P(),
    )
    return jax.shard_map(
        per_device, mesh=finer, in_specs=placed, out_specs=P(tm, None, tok, None), check_vma=False
    )
```

```python
import jax
import jax.numpy as jnp
from jax import lax
from jax.experimental import pallas as pl
from jax.experimental.pallas import tpu as pltpu
from jax.sharding import Mesh
from jax.sharding import PartitionSpec as P

HEADS = 16
SWEEPS = 2
LANES = 128
PLANE_GROUPS = 4
LOG2E = 1.4426950408889634
HALF = ("v", "u", "y")
PLANES = ("w", "v", "u")
VMEM = pl.BlockSpec(memory_space=pltpu.VMEM)
SMEM = pl.BlockSpec(memory_space=pltpu.SMEM)


def shifted(value, axis, shift):
    size = lax.axis_size(axis)
    return lax.ppermute(value, axis, [(i, (i + shift) % size) for i in range(size)])


def call(body, outs, specs, *args, scratch=()):
    return pl.pallas_call(
        body,
        out_shape=outs,
        in_specs=specs,
        out_specs=jax.tree.map(lambda _: VMEM, outs),
        scratch_shapes=list(scratch),
        compiler_params=pltpu.CompilerParams(vmem_limit_bytes=16 * 2**20),
    )(*args)


def normed_rows(rows, shift, scale):
    center = jnp.mean(rows, axis=-1, keepdims=True)
    off = rows - center
    spread = jnp.mean(off * off, axis=-1, keepdims=True)
    normed = off / jnp.sqrt(spread + 1e-06)
    return (normed * (1.0 + scale) + shift).astype(jnp.bfloat16)


def modulation_row(where_ref, step_ref, view_ref, step, part):
    return step_ref[step, part : part + 1, :] + view_ref[where_ref[3 + step], part : part + 1, :]


def enter_body(where_ref, mine_ref, start_mine, peer_ref, step_ref, view_ref, x_ref, start_ref, *mod_refs):
    place = where_ref[0]
    start_ref[...] = jnp.concatenate([start_mine[...], peer_ref[mine_ref.shape[0]]], axis=0)
    steps = mine_ref.shape[0]
    for r in range(steps):
        step = lax.rem(place + r, steps)
        shift = modulation_row(where_ref, step_ref, view_ref, step, 0)
        scale = modulation_row(where_ref, step_ref, view_ref, step, 1)
        rows = jnp.concatenate([mine_ref[step], peer_ref[step]], axis=0)
        x_ref[step] = rows
        mod_refs[r][...] = normed_rows(rows, shift, scale)


def share_place(flip, q, places):
    inner = places // PLANE_GROUPS
    block = q // inner
    return (block + flip * (PLANE_GROUPS - 1 - 2 * block)) * inner + q % inner


def resume_body(
    where_ref, start_ref, mine_before, peer_before, lower_ref, step_ref, view_ref, x_ref, *rest
):
    mod_refs, base_ref = rest[:-1], rest[-1]
    place, flip = where_ref[0], where_ref[1]
    steps = mine_before.shape[0]
    places, share, _ = lower_ref.shape
    for q in range(places):
        base_ref[q * share : (q + 1) * share, :] = lower_ref[share_place(flip, q, places)]
    for r in range(steps):
        step = lax.rem(place + r, steps)
        before = jnp.concatenate([mine_before[step], peer_before[step]], axis=0)
        rows = start_ref[...] + (base_ref[...] + before)
        x_ref[step] = rows
        shift = modulation_row(where_ref, step_ref, view_ref, step, 0)
        scale = modulation_row(where_ref, step_ref, view_ref, step, 1)
        mod_refs[r][...] = normed_rows(rows, shift, scale)


def finish_body(where_ref, start_ref, mine_before, peer_before, mine_lower, peer_lower, out_ref, base_ref):
    flip, core = where_ref[1], where_ref[2]
    places, share, _ = mine_lower.shape
    half = places // 2
    sides = ((core, 0, mine_before, mine_lower), (1 - core, half, peer_before, peer_lower))
    for view, low, before_ref, lower_ref in sides:
        for q in range(half):
            base_ref[q * share : (q + 1) * share, :] = lower_ref[share_place(flip, low + q, places)]
        for step in range(before_ref.shape[0]):
            out_ref[step, view] = start_ref[view] + (base_ref[...] + before_ref[step])


def project_rows(rows, w_ref):
    return jnp.dot(rows, w_ref[...], preferred_element_type=jnp.float32).astype(jnp.bfloat16)


def first_body(a0, w_ref, qkv_ref):
    qkv_ref[...] = project_rows(a0[...], w_ref)


def attend(q_ref, kv_ref, mask_ref, outs):
    width = mask_ref.shape[1]
    part = outs[0].shape[0]
    size = width // HEADS
    tiles = [None] * (width // LANES)
    for h in range(HEADS):
        first = h * size // LANES
        last = ((h + 1) * size - 1) // LANES
        low, high = first * LANES, (last + 1) * LANES
        q = q_ref[:, low:high] * mask_ref[h : h + 1, low:high]
        k = kv_ref[:, width + low : width + high]
        v = kv_ref[:, 2 * width + low : 2 * width + high]
        scores = lax.dot_general(q, k, (((1,), (1,)), ((), ())), preferred_element_type=jnp.float32)
        top = jnp.max(scores, axis=-1, keepdims=True)
        powers = jnp.exp2((scores - top) * (LOG2E / size**0.5))
        share = 1.0 / jnp.sum(powers, axis=-1, keepdims=True)
        out = jnp.dot(powers.astype(jnp.bfloat16), v, preferred_element_type=jnp.float32) * share
        for t in range(first, last + 1):
            piece = out[:, t * LANES - low : (t + 1) * LANES - low]
            if tiles[t] is not None:
                lane = lax.broadcasted_iota(jnp.int32, piece.shape, 1) + t * LANES
                piece = jnp.where(lane >= h * size, piece, tiles[t])
            tiles[t] = piece
    for t, tile in enumerate(tiles):
        tile = tile.astype(jnp.bfloat16)
        for r, out in enumerate(outs):
            out[:, t * LANES : (t + 1) * LANES] = tile[r * part : (r + 1) * part]


def others_body(first_ref, a1, a2, a3, w_ref, mask_ref, o1, o2, o3, qkv_ref, rows_ref):
    part = a1.shape[0]
    for r, piece in enumerate((a1, a2, a3)):
        rows_ref[r * part : (r + 1) * part, :] = piece[...]
    qkv_ref[: 3 * part, :] = project_rows(rows_ref[...], w_ref)
    qkv_ref[3 * part :, :] = first_ref[...]
    attend(qkv_ref.at[: 3 * part], qkv_ref, mask_ref, (o1, o2, o3))


def own_body(first_ref, qkv_ref, mask_ref, o0):
    attend(first_ref, qkv_ref, mask_ref, (o0,))


def base_body(coef_ref, x_ref, mine_ref, peer_ref, base_ref):
    for step in range(x_ref.shape[0]):
        rows = x_ref[step]
        drawn = jnp.concatenate([mine_ref[step], peer_ref[step]], axis=0).astype(jnp.float32)
        base_ref[step] = (coef_ref[0, step] + coef_ref[1, step]) * rows + coef_ref[2, step] * drawn


def project_body(
    where_ref,
    coef_ref,
    a0,
    a1,
    a2,
    a3,
    w_ref,
    base_ref,
    step_ref,
    view_ref,
    mine_before,
    peer_before,
    total_ref,
    rows_ref,
    proj_ref,
):
    place, flip = where_ref[0], where_ref[1]
    pieces = (a0, a1, a2, a3)
    part = a0.shape[0]
    half = part // 2
    steps = len(pieces)
    for r in range(steps):
        rows = pl.ds(pl.multiple_of(lax.rem(place + r, steps) * part, part), part)
        rows_ref[rows, :] = pieces[r][...]
    proj_ref[...] = jnp.dot(rows_ref[...], w_ref[...], preferred_element_type=jnp.float32)
    running = jnp.zeros((part, proj_ref.shape[1]), jnp.float32)
    for step in range(steps):
        gate = modulation_row(where_ref, step_ref, view_ref, step, 2) * coef_ref[1, step]
        mine_before[step] = running[:half]
        peer_before[step] = running[half:]
        running = running + (base_ref[step] + gate * proj_ref[step * part : (step + 1) * part, :])
    places, share, _ = total_ref.shape
    for q in range(places):
        total_ref[share_place(flip, q, places)] = running[q * share : (q + 1) * share]


def coefficients(steps_index):
    unit = steps_index.astype(jnp.float32) / 1000.0
    beta = 0.1 + 19.9 * unit
    sigma = jnp.sqrt(1.0 - jnp.exp(-(0.1 * unit + 9.95 * unit * unit)))
    coef_state = 0.5 * beta * 0.004
    coef_eps = beta * 0.004 / sigma
    coef_noise = jnp.sqrt(beta * 0.004)
    return (coef_state, coef_eps, coef_noise)


def inside_body(held_ref, before_ref, all_ref):
    running = jnp.zeros(held_ref.shape[1:], held_ref.dtype)
    for q in range(held_ref.shape[0]):
        before_ref[q] = running
        running = running + held_ref[q]
    all_ref[...] = running


def below_body(where_ref, before_ref, below_ref, out_ref):
    below = jnp.where(where_ref[1] == 1, below_ref[...], 0.0)
    for q in range(before_ref.shape[0]):
        out_ref[q] = before_ref[q] + below


def earlier_sum(where, shares, beside=None):
    held = lax.all_to_all(shares, HALF, 0, 0, tiled=True)
    whole = jax.ShapeDtypeStruct(shares.shape, shares.dtype)
    before, total = call(inside_body, [whole, jax.ShapeDtypeStruct(shares.shape[1:], shares.dtype)], [VMEM], held)
    planes = lax.axis_size(PLANES)
    below = lax.ppermute(total, PLANES, [(i, planes - 1 - i) for i in range(planes)])
    if beside is not None:
        below, beside = lax.optimization_barrier((below, shifted(beside, "c", 1)))
    sums = call(below_body, whole, [SMEM] + [VMEM] * 2, where, before, below)
    return lax.all_to_all(sums, HALF, 0, 0, tiled=True), beside


def per_device(states, noise, x_start, timesteps, step_mod, view_mod, view_ids, w_qkv, w_out):
    steps, views, part, width = states.shape
    place, flip, core = (lax.axis_index(a) for a in ("x", "w", "c"))
    other = 1 - core
    f32, bf16 = jnp.float32, jnp.bfloat16
    rows = 2 * part

    def own(a, axis):
        return lax.dynamic_index_in_dim(a, core, axis, keepdims=False)

    def given(a, axis):
        return lax.dynamic_index_in_dim(a, other, axis, keepdims=False)

    def shape(*dims, kind=f32):
        return jax.ShapeDtypeStruct(dims, kind)

    swapped = shifted(jnp.concatenate([given(states, 1), given(x_start, 0)[None]], axis=0), "c", 1)
    states_mine, start_mine = own(states, 1), own(x_start, 0)
    noise_mine, noise_peer = own(noise, 1), shifted(given(noise, 1), "c", 1)
    where = jnp.concatenate([jnp.stack([place, flip, core]).astype(jnp.int32), own(view_ids, 1)])
    coefs = jnp.stack(coefficients(timesteps))
    size = width // HEADS
    column = jnp.arange(width, dtype=jnp.int32)[None, :]
    head = jnp.arange(HEADS, dtype=jnp.int32)[:, None]
    mask = ((column >= head * size) & (column < (head + 1) * size)).astype(bf16)

    x_shape = shape(steps, rows, width)
    half = shape(steps, part, width)
    places = lax.axis_size(HALF)
    piece = shape(rows, width, kind=bf16)
    x, start, *mods = call(
        enter_body,
        [x_shape, shape(rows, width)] + [piece] * steps,
        [SMEM] + [VMEM] * 5,
        where,
        states_mine,
        start_mine,
        swapped,
        step_mod,
        view_mod,
    )
    for sweep in range(SWEEPS):
        arrived = [shifted(mods[r], "x", r) for r in range(1, steps)]
        first = call(first_body, shape(rows, 3 * width, kind=bf16), [VMEM] * 2, mods[0], w_qkv)
        *attended, qkv = call(
            others_body,
            [piece] * (steps - 1) + [shape(steps * rows, 3 * width, kind=bf16)],
            [VMEM] * 6,
            first,
            *arrived,
            w_qkv,
            mask,
            scratch=[pltpu.VMEM(((steps - 1) * rows, width), bf16)],
        )
        back = [shifted(attended[r - 1], "x", -r) for r in range(1, steps)]
        kept = call(own_body, piece, [VMEM] * 3, first, qkv, mask)
        base = call(base_body, x_shape, [SMEM] + [VMEM] * 3, coefs, x, noise_mine, noise_peer)
        mine_before, peer_before, total = call(
            project_body,
            [half, half, shape(places, rows // places, width)],
            [SMEM] * 2 + [VMEM] * 8,
            where,
            coefs,
            kept,
            *back,
            w_out,
            base,
            step_mod,
            view_mod,
            scratch=[pltpu.VMEM((steps * rows, width), bf16), pltpu.VMEM((steps * rows, width), f32)],
        )
        if sweep + 1 == SWEEPS:
            break
        lower, _ = earlier_sum(where, total)
        x, *mods = call(
            resume_body,
            [x_shape] + [piece] * steps,
            [SMEM] + [VMEM] * 6,
            where,
            start,
            mine_before,
            peer_before,
            lower,
            step_mod,
            view_mod,
            scratch=[pltpu.VMEM((rows, width), f32)],
        )
    lower, peer_before = earlier_sum(where, total, peer_before)
    return call(
        finish_body,
        shape(*states.shape),
        [SMEM] + [VMEM] * 5,
        where,
        x_start,
        mine_before,
        peer_before,
        lower,
        shifted(lower, "c", 1),
        scratch=[pltpu.VMEM((part, width), f32)],
    )


def solution(mesh):
    finer = Mesh(mesh.devices.reshape(2, 2, 2, 4, 4, 2), ("w", "v", "u", "y", "x", "c"))
    tm, tok = ("w", "v", "u", "y"), ("x", "c")
    placed = (
        P(tm, None, tok, None),
        P(tm, None, tok, None),
        P(None, tok, None),
        P(tm),
        P(tm, None, None),
        P(),
        P(tm, None),
        P(),
        P(),
    )
    return jax.shard_map(
        per_device, mesh=finer, in_specs=placed, out_specs=P(tm, None, tok, None), check_vma=False
    )
```

```python
import jax
import jax.numpy as jnp
from jax import lax
from jax.experimental import pallas as pl
from jax.experimental.pallas import tpu as pltpu
from jax.sharding import Mesh
from jax.sharding import PartitionSpec as P

HEADS = 16
SWEEPS = 2
LANES = 128
LOG2E = 1.4426950408889634
SHARES = ("u", "y")
GROUPS = ("w", "v")
VMEM = pl.BlockSpec(memory_space=pltpu.VMEM)
SMEM = pl.BlockSpec(memory_space=pltpu.SMEM)


def shifted(value, axis, shift):
    size = lax.axis_size(axis)
    return lax.ppermute(value, axis, [(i, (i + shift) % size) for i in range(size)])


def call(body, outs, specs, *args, scratch=()):
    return pl.pallas_call(
        body,
        out_shape=outs,
        in_specs=specs,
        out_specs=jax.tree.map(lambda _: VMEM, outs),
        scratch_shapes=list(scratch),
        compiler_params=pltpu.CompilerParams(vmem_limit_bytes=16 * 2**20),
    )(*args)


def normed_rows(rows, shift, scale):
    center = jnp.mean(rows, axis=-1, keepdims=True)
    off = rows - center
    spread = jnp.mean(off * off, axis=-1, keepdims=True)
    normed = off / jnp.sqrt(spread + 1e-06)
    return (normed * (1.0 + scale) + shift).astype(jnp.bfloat16)


def modulation_row(where_ref, step_ref, view_ref, step, part):
    return step_ref[step, part : part + 1, :] + view_ref[where_ref[3 + step], part : part + 1, :]


def enter_body(where_ref, mine_ref, start_mine, peer_ref, step_ref, view_ref, x_ref, start_ref, *mod_refs):
    place = where_ref[0]
    start_ref[...] = jnp.concatenate([start_mine[...], peer_ref[mine_ref.shape[0]]], axis=0)
    steps = mine_ref.shape[0]
    for r in range(steps):
        step = lax.rem(place + r, steps)
        shift = modulation_row(where_ref, step_ref, view_ref, step, 0)
        scale = modulation_row(where_ref, step_ref, view_ref, step, 1)
        rows = jnp.concatenate([mine_ref[step], peer_ref[step]], axis=0)
        x_ref[step] = rows
        mod_refs[r][...] = normed_rows(rows, shift, scale)


def resume_body(
    where_ref, start_ref, mine_before, peer_before, lower_ref, step_ref, view_ref, x_ref, *rest
):
    mod_refs, base_ref = rest[:-1], rest[-1]
    place = where_ref[0]
    steps = mine_before.shape[0]
    places, share, _ = lower_ref.shape
    for q in range(places):
        base_ref[q * share : (q + 1) * share, :] = lower_ref[q]
    for r in range(steps):
        step = lax.rem(place + r, steps)
        before = jnp.concatenate([mine_before[step], peer_before[step]], axis=0)
        rows = start_ref[...] + (base_ref[...] + before)
        x_ref[step] = rows
        shift = modulation_row(where_ref, step_ref, view_ref, step, 0)
        scale = modulation_row(where_ref, step_ref, view_ref, step, 1)
        mod_refs[r][...] = normed_rows(rows, shift, scale)


def finish_body(where_ref, start_ref, mine_before, peer_before, mine_lower, peer_lower, out_ref, base_ref):
    core = where_ref[2]
    places, share, _ = mine_lower.shape
    half = places // 2
    sides = ((core, 0, mine_before, mine_lower), (1 - core, half, peer_before, peer_lower))
    for view, low, before_ref, lower_ref in sides:
        for q in range(half):
            base_ref[q * share : (q + 1) * share, :] = lower_ref[low + q]
        for step in range(before_ref.shape[0]):
            out_ref[step, view] = start_ref[view] + (base_ref[...] + before_ref[step])


def project_rows(rows, w_ref):
    return jnp.dot(rows, w_ref[...], preferred_element_type=jnp.float32).astype(jnp.bfloat16)


def first_body(a0, w_ref, qkv_ref):
    qkv_ref[...] = project_rows(a0[...], w_ref)


def attend(q_ref, kv_ref, mask_ref, outs):
    width = mask_ref.shape[1]
    part = outs[0].shape[0]
    size = width // HEADS
    tiles = [None] * (width // LANES)
    for h in range(HEADS):
        first = h * size // LANES
        last = ((h + 1) * size - 1) // LANES
        low, high = first * LANES, (last + 1) * LANES
        q = q_ref[:, low:high] * mask_ref[h : h + 1, low:high]
        k = kv_ref[:, width + low : width + high]
        v = kv_ref[:, 2 * width + low : 2 * width + high]
        scores = lax.dot_general(q, k, (((1,), (1,)), ((), ())), preferred_element_type=jnp.float32)
        top = jnp.max(scores, axis=-1, keepdims=True)
        powers = jnp.exp2((scores - top) * (LOG2E / size**0.5))
        share = 1.0 / jnp.sum(powers, axis=-1, keepdims=True)
        out = jnp.dot(powers.astype(jnp.bfloat16), v, preferred_element_type=jnp.float32) * share
        for t in range(first, last + 1):
            piece = out[:, t * LANES - low : (t + 1) * LANES - low]
            if tiles[t] is not None:
                lane = lax.broadcasted_iota(jnp.int32, piece.shape, 1) + t * LANES
                piece = jnp.where(lane >= h * size, piece, tiles[t])
            tiles[t] = piece
    for t, tile in enumerate(tiles):
        tile = tile.astype(jnp.bfloat16)
        for r, out in enumerate(outs):
            out[:, t * LANES : (t + 1) * LANES] = tile[r * part : (r + 1) * part]


def others_body(first_ref, a1, a2, a3, w_ref, mask_ref, o1, o2, o3, qkv_ref, rows_ref):
    part = a1.shape[0]
    for r, piece in enumerate((a1, a2, a3)):
        rows_ref[r * part : (r + 1) * part, :] = piece[...]
    qkv_ref[: 3 * part, :] = project_rows(rows_ref[...], w_ref)
    qkv_ref[3 * part :, :] = first_ref[...]
    attend(qkv_ref.at[: 3 * part], qkv_ref, mask_ref, (o1, o2, o3))


def own_body(first_ref, qkv_ref, mask_ref, o0):
    attend(first_ref, qkv_ref, mask_ref, (o0,))


def base_body(coef_ref, x_ref, mine_ref, peer_ref, base_ref):
    for step in range(x_ref.shape[0]):
        rows = x_ref[step]
        drawn = jnp.concatenate([mine_ref[step], peer_ref[step]], axis=0).astype(jnp.float32)
        base_ref[step] = (coef_ref[0, step] + coef_ref[1, step]) * rows + coef_ref[2, step] * drawn


def project_body(
    where_ref,
    coef_ref,
    a0,
    a1,
    a2,
    a3,
    w_ref,
    base_ref,
    step_ref,
    view_ref,
    mine_before,
    peer_before,
    total_ref,
    rows_ref,
    proj_ref,
):
    place = where_ref[0]
    pieces = (a0, a1, a2, a3)
    part = a0.shape[0]
    half = part // 2
    steps = len(pieces)
    for r in range(steps):
        rows = pl.ds(pl.multiple_of(lax.rem(place + r, steps) * part, part), part)
        rows_ref[rows, :] = pieces[r][...]
    proj_ref[...] = jnp.dot(rows_ref[...], w_ref[...], preferred_element_type=jnp.float32)
    running = jnp.zeros((part, proj_ref.shape[1]), jnp.float32)
    for step in range(steps):
        gate = modulation_row(where_ref, step_ref, view_ref, step, 2) * coef_ref[1, step]
        mine_before[step] = running[:half]
        peer_before[step] = running[half:]
        running = running + (base_ref[step] + gate * proj_ref[step * part : (step + 1) * part, :])
    places, share, _ = total_ref.shape
    for q in range(places):
        total_ref[q] = running[q * share : (q + 1) * share]


def coefficients(steps_index):
    unit = steps_index.astype(jnp.float32) / 1000.0
    beta = 0.1 + 19.9 * unit
    sigma = jnp.sqrt(1.0 - jnp.exp(-(0.1 * unit + 9.95 * unit * unit)))
    coef_state = 0.5 * beta * 0.004
    coef_eps = beta * 0.004 / sigma
    coef_noise = jnp.sqrt(beta * 0.004)
    return (coef_state, coef_eps, coef_noise)


def inside_body(held_ref, before_ref, all_ref):
    running = jnp.zeros(held_ref.shape[1:], held_ref.dtype)
    for q in range(held_ref.shape[0]):
        before_ref[q] = running
        running = running + held_ref[q]
    all_ref[...] = running


def below_body(where_ref, before_ref, *refs):
    passed, out_ref = refs[:-1], refs[-1]
    group = where_ref[1]
    below = jnp.zeros(before_ref.shape[1:], before_ref.dtype)
    for shift, ref in enumerate(passed, 1):
        below = below + jnp.where(shift <= group, ref[...], 0.0)
    for q in range(before_ref.shape[0]):
        out_ref[q] = before_ref[q] + below


def earlier_sum(where, shares, beside=None):
    held = lax.all_to_all(shares, SHARES, 0, 0, tiled=True)
    whole = jax.ShapeDtypeStruct(shares.shape, shares.dtype)
    before, total = call(inside_body, [whole, jax.ShapeDtypeStruct(shares.shape[1:], shares.dtype)], [VMEM], held)
    passed = [shifted(total, GROUPS, shift) for shift in range(1, lax.axis_size(GROUPS))]
    if beside is not None:
        passed[0], beside = lax.optimization_barrier((passed[0], shifted(beside, "c", 1)))
    sums = call(below_body, whole, [SMEM] + [VMEM] * (1 + len(passed)), where, before, *passed)
    return lax.all_to_all(sums, SHARES, 0, 0, tiled=True), beside


def per_device(states, noise, x_start, timesteps, step_mod, view_mod, view_ids, w_qkv, w_out):
    steps, views, part, width = states.shape
    place, group, core = (lax.axis_index(a) for a in ("x", GROUPS, "c"))
    other = 1 - core
    f32, bf16 = jnp.float32, jnp.bfloat16
    rows = 2 * part

    def own(a, axis):
        return lax.dynamic_index_in_dim(a, core, axis, keepdims=False)

    def given(a, axis):
        return lax.dynamic_index_in_dim(a, other, axis, keepdims=False)

    def shape(*dims, kind=f32):
        return jax.ShapeDtypeStruct(dims, kind)

    swapped = shifted(jnp.concatenate([given(states, 1), given(x_start, 0)[None]], axis=0), "c", 1)
    states_mine, start_mine = own(states, 1), own(x_start, 0)
    noise_mine, noise_peer = own(noise, 1), shifted(given(noise, 1), "c", 1)
    where = jnp.concatenate([jnp.stack([place, group, core]).astype(jnp.int32), own(view_ids, 1)])
    coefs = jnp.stack(coefficients(timesteps))
    size = width // HEADS
    column = jnp.arange(width, dtype=jnp.int32)[None, :]
    head = jnp.arange(HEADS, dtype=jnp.int32)[:, None]
    mask = ((column >= head * size) & (column < (head + 1) * size)).astype(bf16)

    x_shape = shape(steps, rows, width)
    half = shape(steps, part, width)
    places = lax.axis_size(SHARES)
    piece = shape(rows, width, kind=bf16)
    x, start, *mods = call(
        enter_body,
        [x_shape, shape(rows, width)] + [piece] * steps,
        [SMEM] + [VMEM] * 5,
        where,
        states_mine,
        start_mine,
        swapped,
        step_mod,
        view_mod,
    )
    for sweep in range(SWEEPS):
        arrived = [shifted(mods[r], "x", r) for r in range(1, steps)]
        first = call(first_body, shape(rows, 3 * width, kind=bf16), [VMEM] * 2, mods[0], w_qkv)
        *attended, qkv = call(
            others_body,
            [piece] * (steps - 1) + [shape(steps * rows, 3 * width, kind=bf16)],
            [VMEM] * 6,
            first,
            *arrived,
            w_qkv,
            mask,
            scratch=[pltpu.VMEM(((steps - 1) * rows, width), bf16)],
        )
        back = [shifted(attended[r - 1], "x", -r) for r in range(1, steps)]
        kept = call(own_body, piece, [VMEM] * 3, first, qkv, mask)
        base = call(base_body, x_shape, [SMEM] + [VMEM] * 3, coefs, x, noise_mine, noise_peer)
        mine_before, peer_before, total = call(
            project_body,
            [half, half, shape(places, rows // places, width)],
            [SMEM] * 2 + [VMEM] * 8,
            where,
            coefs,
            kept,
            *back,
            w_out,
            base,
            step_mod,
            view_mod,
            scratch=[pltpu.VMEM((steps * rows, width), bf16), pltpu.VMEM((steps * rows, width), f32)],
        )
        if sweep + 1 == SWEEPS:
            break
        lower, _ = earlier_sum(where, total)
        x, *mods = call(
            resume_body,
            [x_shape] + [piece] * steps,
            [SMEM] + [VMEM] * 6,
            where,
            start,
            mine_before,
            peer_before,
            lower,
            step_mod,
            view_mod,
            scratch=[pltpu.VMEM((rows, width), f32)],
        )
    lower, peer_before = earlier_sum(where, total, peer_before)
    return call(
        finish_body,
        shape(*states.shape),
        [SMEM] + [VMEM] * 5,
        where,
        x_start,
        mine_before,
        peer_before,
        lower,
        shifted(lower, "c", 1),
        scratch=[pltpu.VMEM((part, width), f32)],
    )


def solution(mesh):
    finer = Mesh(mesh.devices.reshape(2, 2, 2, 4, 4, 2), ("w", "v", "u", "y", "x", "c"))
    tm, tok = ("w", "v", "u", "y"), ("x", "c")
    placed = (
        P(tm, None, tok, None),
        P(tm, None, tok, None),
        P(None, tok, None),
        P(tm),
        P(tm, None, None),
        P(),
        P(tm, None),
        P(),
        P(),
    )
    return jax.shard_map(
        per_device, mesh=finer, in_specs=placed, out_specs=P(tm, None, tok, None), check_vma=False
    )
```

```python
import jax
import jax.numpy as jnp
from jax import lax
from jax.experimental import pallas as pl
from jax.experimental.pallas import tpu as pltpu
from jax.sharding import Mesh
from jax.sharding import PartitionSpec as P


HEADS = 16
SWEEPS = 2
LANES = 128
LOG2E = 1.4426950408889634
SHARES = ("u", "y")
GROUPS = ("w", "v")
VMEM = pl.BlockSpec(memory_space=pltpu.VMEM)
SMEM = pl.BlockSpec(memory_space=pltpu.SMEM)


def shifted(value, axis, shift):
    size = lax.axis_size(axis)
    return lax.ppermute(value, axis, [(i, (i + shift) % size) for i in range(size)])


def spread(values, axis, sign=1):
    moved = []
    for k, value in enumerate(values, 1):
        moved.append(shifted(value, axis, sign * k))
    return moved


def call(body, outs, specs, *args, scratch=(), out_spec=VMEM):
    return pl.pallas_call(
        body,
        out_shape=outs,
        in_specs=specs,
        out_specs=jax.tree.map(lambda _: out_spec, outs),
        scratch_shapes=list(scratch),
        compiler_params=pltpu.CompilerParams(vmem_limit_bytes=16 * 2**20),
    )(*args)


def normed_rows(rows, shift, scale):
    center = jnp.mean(rows, axis=-1, keepdims=True)
    off = rows - center
    spread = jnp.mean(off * off, axis=-1, keepdims=True)
    normed = off / jnp.sqrt(spread + 1e-06)
    return (normed * (1.0 + scale) + shift).astype(jnp.bfloat16)


def modulation_row(where_ref, step_ref, view_ref, step, part):
    return step_ref[step, part : part + 1, :] + view_ref[where_ref[3 + step], part : part + 1, :]


def enter_body(where_ref, mine_ref, start_mine, peer_ref, step_ref, view_ref, x_ref, start_ref, *mod_refs):
    place = where_ref[0]
    start_ref[...] = jnp.concatenate([start_mine[...], peer_ref[mine_ref.shape[0]]], axis=0)
    steps = mine_ref.shape[0]
    for r in range(steps):
        step = lax.rem(place + r, steps)
        shift = modulation_row(where_ref, step_ref, view_ref, step, 0)
        scale = modulation_row(where_ref, step_ref, view_ref, step, 1)
        rows = jnp.concatenate([mine_ref[step], peer_ref[step]], axis=0)
        x_ref[step] = rows
        mod_refs[r][...] = normed_rows(rows, shift, scale)


def resume_body(
    where_ref, start_ref, mine_before, peer_before, lower_ref, step_ref, view_ref, x_ref, *rest
):
    mod_refs, base_ref = rest[:-1], rest[-1]
    place = where_ref[0]
    steps = mine_before.shape[0]
    places, share, _ = lower_ref.shape
    for q in range(places):
        base_ref[q * share : (q + 1) * share, :] = lower_ref[q]
    for r in range(steps):
        step = lax.rem(place + r, steps)
        before = jnp.concatenate([mine_before[step], peer_before[step]], axis=0)
        rows = start_ref[...] + (base_ref[...] + before)
        x_ref[step] = rows
        shift = modulation_row(where_ref, step_ref, view_ref, step, 0)
        scale = modulation_row(where_ref, step_ref, view_ref, step, 1)
        mod_refs[r][...] = normed_rows(rows, shift, scale)


def finish_body(
    where_ref, start_ref, mine_before, peer_before, mine_lower, peer_lower, out_ref, base_ref, rows_ref, sems
):
    core = where_ref[2]
    places, share, _ = mine_lower.shape
    half = places // 2
    sides = ((core, 0, mine_before, mine_lower), (1 - core, half, peer_before, peer_lower))
    copies = []
    for side, (view, low, before_ref, lower_ref) in enumerate(sides):
        for q in range(half):
            rows = slice(q * share, (q + 1) * share)
            base_ref[rows, :] = lower_ref[low + q]
        for step in range(before_ref.shape[0]):
            rows_ref[side, step] = start_ref[view] + (base_ref[...] + before_ref[step])
            copies.append(
                pltpu.make_async_copy(rows_ref.at[side, step], out_ref.at[step, view], sems.at[side, step])
            )
            copies[-1].start()
    for copy in copies:
        copy.wait()


def project_rows(rows, w_ref):
    return jnp.dot(rows, w_ref[...], preferred_element_type=jnp.float32).astype(jnp.bfloat16)


def first_body(a0, w_ref, qkv_ref):
    qkv_ref[...] = project_rows(a0[...], w_ref)


def attend(q_ref, kv_ref, mask_ref, outs):
    width = mask_ref.shape[1]
    part = outs[0].shape[0]
    size = width // HEADS
    tiles = [None] * (width // LANES)
    for h in range(HEADS):
        first = h * size // LANES
        last = ((h + 1) * size - 1) // LANES
        low, high = first * LANES, (last + 1) * LANES
        q = q_ref[:, low:high] * mask_ref[h : h + 1, low:high]
        k = kv_ref[:, width + low : width + high]
        v = kv_ref[:, 2 * width + low : 2 * width + high]
        scores = lax.dot_general(q, k, (((1,), (1,)), ((), ())), preferred_element_type=jnp.float32)
        top = jnp.max(scores, axis=-1, keepdims=True)
        powers = jnp.exp2((scores - top) * (LOG2E / size**0.5))
        share = 1.0 / jnp.sum(powers, axis=-1, keepdims=True)
        out = jnp.dot(powers.astype(jnp.bfloat16), v, preferred_element_type=jnp.float32) * share
        for t in range(first, last + 1):
            piece = out[:, t * LANES - low : (t + 1) * LANES - low]
            if tiles[t] is not None:
                lane = lax.broadcasted_iota(jnp.int32, piece.shape, 1) + t * LANES
                piece = jnp.where(lane >= h * size, piece, tiles[t])
            tiles[t] = piece
    for t, tile in enumerate(tiles):
        tile = tile.astype(jnp.bfloat16)
        for r, out in enumerate(outs):
            out[:, t * LANES : (t + 1) * LANES] = tile[r * part : (r + 1) * part]


def others_body(first_ref, a1, a2, a3, w_ref, mask_ref, o1, o2, o3, qkv_ref, rows_ref):
    part = a1.shape[0]
    for r, piece in enumerate((a1, a2, a3)):
        rows_ref[r * part : (r + 1) * part, :] = piece[...]
    qkv_ref[: 3 * part, :] = project_rows(rows_ref[...], w_ref)
    qkv_ref[3 * part :, :] = first_ref[...]
    attend(qkv_ref.at[: 3 * part], qkv_ref, mask_ref, (o1, o2, o3))


def own_body(first_ref, qkv_ref, mask_ref, o0):
    attend(first_ref, qkv_ref, mask_ref, (o0,))


def base_body(coef_ref, x_ref, mine_ref, peer_ref, base_ref):
    for step in range(x_ref.shape[0]):
        rows = x_ref[step]
        drawn = jnp.concatenate([mine_ref[step], peer_ref[step]], axis=0).astype(jnp.float32)
        base_ref[step] = (coef_ref[0, step] + coef_ref[1, step]) * rows + coef_ref[2, step] * drawn


def project_body(
    where_ref,
    coef_ref,
    a0,
    a1,
    a2,
    a3,
    w_ref,
    base_ref,
    step_ref,
    view_ref,
    mine_before,
    peer_before,
    total_ref,
    rows_ref,
    proj_ref,
):
    place = where_ref[0]
    pieces = (a0, a1, a2, a3)
    part = a0.shape[0]
    half = part // 2
    steps = len(pieces)
    for r in range(steps):
        rows = pl.ds(pl.multiple_of(lax.rem(place + r, steps) * part, part), part)
        rows_ref[rows, :] = pieces[r][...]
    proj_ref[...] = jnp.dot(rows_ref[...], w_ref[...], preferred_element_type=jnp.float32)
    running = jnp.zeros((part, proj_ref.shape[1]), jnp.float32)
    for step in range(steps):
        gate = modulation_row(where_ref, step_ref, view_ref, step, 2) * coef_ref[1, step]
        mine_before[step] = running[:half]
        peer_before[step] = running[half:]
        running = running + (base_ref[step] + gate * proj_ref[step * part : (step + 1) * part, :])
    places, share, _ = total_ref.shape
    for q in range(places):
        total_ref[q] = running[q * share : (q + 1) * share]


def coefficients(steps_index):
    unit = steps_index.astype(jnp.float32) / 1000.0
    beta = 0.1 + 19.9 * unit
    sigma = jnp.sqrt(1.0 - jnp.exp(-(0.1 * unit + 9.95 * unit * unit)))
    coef_state = 0.5 * beta * 0.004
    coef_eps = beta * 0.004 / sigma
    coef_noise = jnp.sqrt(beta * 0.004)
    return (coef_state, coef_eps, coef_noise)


def inside_body(held_ref, before_ref, all_ref):
    running = jnp.zeros(held_ref.shape[1:], held_ref.dtype)
    for q in range(held_ref.shape[0]):
        before_ref[q] = running
        running = running + held_ref[q]
    all_ref[...] = running


def below_body(where_ref, before_ref, *refs):
    passed, out_ref = refs[:-1], refs[-1]
    group = where_ref[1]
    below = jnp.zeros(before_ref.shape[1:], before_ref.dtype)
    for shift, ref in enumerate(passed, 1):
        below = below + jnp.where(shift <= group, ref[...], 0.0)
    for q in range(before_ref.shape[0]):
        out_ref[q] = before_ref[q] + below


def earlier_sum(where, shares, beside=None):
    held = lax.all_to_all(shares, SHARES, 0, 0, tiled=True)
    whole = jax.ShapeDtypeStruct(shares.shape, shares.dtype)
    before, total = call(inside_body, [whole, jax.ShapeDtypeStruct(shares.shape[1:], shares.dtype)], [VMEM], held)
    passed = spread([total] * (lax.axis_size(GROUPS) - 1), GROUPS)
    if beside is not None:
        passed[0], beside = lax.optimization_barrier((passed[0], shifted(beside, "c", 1)))
    sums = call(below_body, whole, [SMEM] + [VMEM] * (1 + len(passed)), where, before, *passed)
    return lax.all_to_all(sums, SHARES, 0, 0, tiled=True), beside


def device_program(states, noise, x_start, timesteps, step_mod, view_mod, view_ids, w_qkv, w_out):
    steps, views, part, width = states.shape
    place, group, core = (lax.axis_index(a) for a in ("x", GROUPS, "c"))
    other = 1 - core
    f32, bf16 = jnp.float32, jnp.bfloat16
    rows = 2 * part

    def own(a, axis):
        return lax.dynamic_index_in_dim(a, core, axis, keepdims=False)

    def given(a, axis):
        return lax.dynamic_index_in_dim(a, other, axis, keepdims=False)

    def shape(*dims, kind=f32):
        return jax.ShapeDtypeStruct(dims, kind)

    swapped = shifted(jnp.concatenate([given(states, 1), given(x_start, 0)[None]], axis=0), "c", 1)
    states_mine, start_mine = own(states, 1), own(x_start, 0)
    where = jnp.concatenate([jnp.stack([place, group, core]).astype(jnp.int32), own(view_ids, 1)])
    coefs = jnp.stack(coefficients(timesteps))
    size = width // HEADS
    column = jnp.arange(width, dtype=jnp.int32)[None, :]
    head = jnp.arange(HEADS, dtype=jnp.int32)[:, None]
    mask = ((column >= head * size) & (column < (head + 1) * size)).astype(bf16)

    x_shape = shape(steps, rows, width)
    half = shape(steps, part, width)
    places = lax.axis_size(SHARES)
    piece = shape(rows, width, kind=bf16)
    x, start, *mods = call(
        enter_body,
        [x_shape, shape(rows, width)] + [piece] * steps,
        [SMEM] + [VMEM] * 5,
        where,
        states_mine,
        start_mine,
        swapped,
        step_mod,
        view_mod,
    )
    drawn, _ = lax.optimization_barrier((noise, mods[0]))
    noise_mine, noise_peer = own(drawn, 1), shifted(given(drawn, 1), "c", 1)
    for sweep in range(SWEEPS):
        arrived = spread(mods[1:], "x")
        first = call(first_body, shape(rows, 3 * width, kind=bf16), [VMEM] * 2, mods[0], w_qkv)
        *attended, qkv = call(
            others_body,
            [piece] * (steps - 1) + [shape(steps * rows, 3 * width, kind=bf16)],
            [VMEM] * 6,
            first,
            *arrived,
            w_qkv,
            mask,
            scratch=[pltpu.VMEM(((steps - 1) * rows, width), bf16)],
        )
        back = spread(attended, "x", -1)
        kept = call(own_body, piece, [VMEM] * 3, first, qkv, mask)
        base = call(base_body, x_shape, [SMEM] + [VMEM] * 3, coefs, x, noise_mine, noise_peer)
        mine_before, peer_before, total = call(
            project_body,
            [half, half, shape(places, rows // places, width)],
            [SMEM] * 2 + [VMEM] * 8,
            where,
            coefs,
            kept,
            *back,
            w_out,
            base,
            step_mod,
            view_mod,
            scratch=[pltpu.VMEM((steps * rows, width), bf16), pltpu.VMEM((steps * rows, width), f32)],
        )
        if sweep + 1 == SWEEPS:
            break
        lower, _ = earlier_sum(where, total)
        x, *mods = call(
            resume_body,
            [x_shape] + [piece] * steps,
            [SMEM] + [VMEM] * 6,
            where,
            start,
            mine_before,
            peer_before,
            lower,
            step_mod,
            view_mod,
            scratch=[pltpu.VMEM((rows, width), f32)],
        )
    lower, peer_before = earlier_sum(where, total, peer_before)
    return call(
        finish_body,
        shape(*states.shape),
        [SMEM] + [VMEM] * 5,
        where,
        x_start,
        mine_before,
        peer_before,
        lower,
        shifted(lower, "c", 1),
        scratch=[
            pltpu.VMEM((part, width), f32),
            pltpu.VMEM((views, steps, part, width), f32),
            pltpu.SemaphoreType.DMA((views, steps)),
        ],
        out_spec=pl.BlockSpec(memory_space=pl.ANY),
    )


def solution(mesh):
    finer = Mesh(mesh.devices.reshape(2, 2, 2, 4, 4, 2), ("w", "v", "u", "y", "x", "c"))
    tm, tok = ("w", "v", "u", "y"), ("x", "c")
    placed = (
        P(tm, None, tok, None),
        P(tm, None, tok, None),
        P(None, tok, None),
        P(tm),
        P(tm, None, None),
        P(),
        P(tm, None),
        P(),
        P(),
    )
    return jax.shard_map(
        device_program, mesh=finer, in_specs=placed, out_specs=P(tm, None, tok, None), check_vma=False
    )
```

```python
import jax
import jax.numpy as jnp
from jax import lax
from jax.experimental import pallas as pl
from jax.experimental.pallas import tpu as pltpu
from jax.sharding import Mesh
from jax.sharding import PartitionSpec as P


HEADS = 16
SWEEPS = 2
LANES = 128
LOG2E = 1.4426950408889634
SHARES = ("u", "y")
GROUPS = ("w", "v")
VMEM = pl.BlockSpec(memory_space=pltpu.VMEM)
SMEM = pl.BlockSpec(memory_space=pltpu.SMEM)


def shifted(value, axis, shift):
    size = lax.axis_size(axis)
    return lax.ppermute(value, axis, [(i, (i + shift) % size) for i in range(size)])


def spread(values, axis, sign=1):
    moved = []
    for k, value in enumerate(values, 1):
        moved.append(shifted(value, axis, sign * k))
    return moved


def call(body, outs, specs, *args, scratch=(), out_spec=VMEM):
    return pl.pallas_call(
        body,
        out_shape=outs,
        in_specs=specs,
        out_specs=jax.tree.map(lambda _: out_spec, outs),
        scratch_shapes=list(scratch),
        compiler_params=pltpu.CompilerParams(vmem_limit_bytes=16 * 2**20),
    )(*args)


def normed_rows(rows, shift, scale):
    center = jnp.mean(rows, axis=-1, keepdims=True)
    off = rows - center
    spread = jnp.mean(off * off, axis=-1, keepdims=True)
    normed = off / jnp.sqrt(spread + 1e-06)
    return (normed * (1.0 + scale) + shift).astype(jnp.bfloat16)


def modulation_row(where_ref, step_ref, view_ref, step, part):
    return step_ref[step, part : part + 1, :] + view_ref[where_ref[3 + step], part : part + 1, :]


def enter_body(where_ref, mine_ref, start_mine, peer_ref, step_ref, view_ref, x_ref, start_ref, *mod_refs):
    place = where_ref[0]
    start_ref[...] = jnp.concatenate([start_mine[...], peer_ref[mine_ref.shape[0]]], axis=0)
    steps = mine_ref.shape[0]
    for r in range(steps):
        step = lax.rem(place + r, steps)
        shift = modulation_row(where_ref, step_ref, view_ref, step, 0)
        scale = modulation_row(where_ref, step_ref, view_ref, step, 1)
        rows = jnp.concatenate([mine_ref[step], peer_ref[step]], axis=0)
        x_ref[step] = rows
        mod_refs[r][...] = normed_rows(rows, shift, scale)


def resume_body(
    where_ref, start_ref, mine_before, peer_before, lower_ref, step_ref, view_ref, x_ref, *rest
):
    mod_refs, base_ref = rest[:-1], rest[-1]
    place = where_ref[0]
    steps = mine_before.shape[0]
    places, share, _ = lower_ref.shape
    for q in range(places):
        base_ref[q * share : (q + 1) * share, :] = lower_ref[q]
    for r in range(steps):
        step = lax.rem(place + r, steps)
        before = jnp.concatenate([mine_before[step], peer_before[step]], axis=0)
        rows = start_ref[...] + (base_ref[...] + before)
        x_ref[step] = rows
        shift = modulation_row(where_ref, step_ref, view_ref, step, 0)
        scale = modulation_row(where_ref, step_ref, view_ref, step, 1)
        mod_refs[r][...] = normed_rows(rows, shift, scale)


def finish_body(
    where_ref, start_ref, mine_before, peer_before, mine_lower, peer_lower, out_ref, base_ref, rows_ref, sems
):
    core = where_ref[2]
    places, share, _ = mine_lower.shape
    half = places // 2
    sides = ((core, 0, mine_before, mine_lower), (1 - core, half, peer_before, peer_lower))
    copies = []
    for side, (view, low, before_ref, lower_ref) in enumerate(sides):
        for q in range(half):
            rows = slice(q * share, (q + 1) * share)
            base_ref[rows, :] = lower_ref[low + q]
        for step in range(before_ref.shape[0]):
            rows_ref[side, step] = start_ref[view] + (base_ref[...] + before_ref[step])
            copies.append(
                pltpu.make_async_copy(rows_ref.at[side, step], out_ref.at[step, view], sems.at[side, step])
            )
            copies[-1].start()
    for copy in copies:
        copy.wait()


def project_rows(rows, w_ref):
    return jnp.dot(rows, w_ref[...], preferred_element_type=jnp.float32).astype(jnp.bfloat16)


def first_body(a0, w_ref, qkv_ref):
    qkv_ref[...] = project_rows(a0[...], w_ref)


def attend(q_ref, kv_ref, mask_ref, outs):
    width = mask_ref.shape[1]
    part = outs[0].shape[0]
    size = width // HEADS
    tiles = [None] * (width // LANES)
    for h in range(HEADS):
        first = h * size // LANES
        last = ((h + 1) * size - 1) // LANES
        low, high = first * LANES, (last + 1) * LANES
        q = q_ref[:, low:high] * mask_ref[h : h + 1, low:high]
        k = kv_ref[:, width + low : width + high]
        v = kv_ref[:, 2 * width + low : 2 * width + high]
        scores = lax.dot_general(q, k, (((1,), (1,)), ((), ())), preferred_element_type=jnp.float32)
        top = jnp.max(scores, axis=-1, keepdims=True)
        powers = jnp.exp2((scores - top) * (LOG2E / size**0.5))
        share = 1.0 / jnp.sum(powers, axis=-1, keepdims=True)
        out = jnp.dot(powers.astype(jnp.bfloat16), v, preferred_element_type=jnp.float32) * share
        for t in range(first, last + 1):
            piece = out[:, t * LANES - low : (t + 1) * LANES - low]
            if tiles[t] is not None:
                lane = lax.broadcasted_iota(jnp.int32, piece.shape, 1) + t * LANES
                piece = jnp.where(lane >= h * size, piece, tiles[t])
            tiles[t] = piece
    for t, tile in enumerate(tiles):
        tile = tile.astype(jnp.bfloat16)
        for r, out in enumerate(outs):
            out[:, t * LANES : (t + 1) * LANES] = tile[r * part : (r + 1) * part]


def others_body(first_ref, a1, a2, a3, w_ref, mask_ref, o1, o2, o3, qkv_ref, rows_ref):
    part = a1.shape[0]
    for r, piece in enumerate((a1, a2, a3)):
        rows_ref[r * part : (r + 1) * part, :] = piece[...]
    qkv_ref[: 3 * part, :] = project_rows(rows_ref[...], w_ref)
    qkv_ref[3 * part :, :] = first_ref[...]
    attend(qkv_ref.at[: 3 * part], qkv_ref, mask_ref, (o1, o2, o3))


def own_body(first_ref, qkv_ref, mask_ref, o0):
    attend(first_ref, qkv_ref, mask_ref, (o0,))


def base_body(coef_ref, x_ref, mine_ref, peer_ref, base_ref):
    for step in range(x_ref.shape[0]):
        rows = x_ref[step]
        drawn = jnp.concatenate([mine_ref[step], peer_ref[step]], axis=0).astype(jnp.float32)
        base_ref[step] = (coef_ref[0, step] + coef_ref[1, step]) * rows + coef_ref[2, step] * drawn


def project_body(
    where_ref,
    coef_ref,
    a0,
    a1,
    a2,
    a3,
    w_ref,
    base_ref,
    step_ref,
    view_ref,
    mine_before,
    peer_before,
    total_ref,
    rows_ref,
    proj_ref,
):
    place = where_ref[0]
    pieces = (a0, a1, a2, a3)
    part = a0.shape[0]
    half = part // 2
    steps = len(pieces)
    for r in range(steps):
        rows = pl.ds(pl.multiple_of(lax.rem(place + r, steps) * part, part), part)
        rows_ref[rows, :] = pieces[r][...]
    proj_ref[...] = jnp.dot(rows_ref[...], w_ref[...], preferred_element_type=jnp.float32)
    running = jnp.zeros((part, proj_ref.shape[1]), jnp.float32)
    for step in range(steps):
        gate = modulation_row(where_ref, step_ref, view_ref, step, 2) * coef_ref[1, step]
        mine_before[step] = running[:half]
        peer_before[step] = running[half:]
        running = running + (base_ref[step] + gate * proj_ref[step * part : (step + 1) * part, :])
    places, share, _ = total_ref.shape
    for q in range(places):
        total_ref[q] = running[q * share : (q + 1) * share]


def coefficients(steps_index):
    unit = steps_index.astype(jnp.float32) / 1000.0
    beta = 0.1 + 19.9 * unit
    sigma = jnp.sqrt(1.0 - jnp.exp(-(0.1 * unit + 9.95 * unit * unit)))
    coef_state = 0.5 * beta * 0.004
    coef_eps = beta * 0.004 / sigma
    coef_noise = jnp.sqrt(beta * 0.004)
    return (coef_state, coef_eps, coef_noise)


def inside_body(held_ref, before_ref, all_ref):
    running = jnp.zeros(held_ref.shape[1:], held_ref.dtype)
    for q in range(held_ref.shape[0]):
        before_ref[q] = running
        running = running + held_ref[q]
    for g in range(all_ref.shape[0]):
        all_ref[g] = running


def below_body(where_ref, before_ref, totals_ref, out_ref):
    group = where_ref[1]
    below = jnp.zeros(before_ref.shape[1:], before_ref.dtype)
    for g in range(totals_ref.shape[0] - 1):
        below = below + jnp.where(g < group, totals_ref[g], 0.0)
    for q in range(before_ref.shape[0]):
        out_ref[q] = before_ref[q] + below


def earlier_sum(where, shares, beside=None):
    held = lax.all_to_all(shares, SHARES, 0, 0, tiled=True)
    whole = jax.ShapeDtypeStruct(shares.shape, shares.dtype)
    copies = jax.ShapeDtypeStruct((lax.axis_size(GROUPS),) + shares.shape[1:], shares.dtype)
    before, total = call(inside_body, [whole, copies], [VMEM], held)
    totals = lax.all_to_all(total, GROUPS, 0, 0, tiled=True)
    sums = call(below_body, whole, [SMEM] + [VMEM] * 2, where, before, totals)
    if beside is not None:
        sums, beside = lax.optimization_barrier((sums, shifted(beside, "c", 1)))
    return lax.all_to_all(sums, SHARES, 0, 0, tiled=True), beside


def device_program(states, noise, x_start, timesteps, step_mod, view_mod, view_ids, w_qkv, w_out):
    steps, views, part, width = states.shape
    place, group, core = (lax.axis_index(a) for a in ("x", GROUPS, "c"))
    other = 1 - core
    f32, bf16 = jnp.float32, jnp.bfloat16
    rows = 2 * part

    def own(a, axis):
        return lax.dynamic_index_in_dim(a, core, axis, keepdims=False)

    def given(a, axis):
        return lax.dynamic_index_in_dim(a, other, axis, keepdims=False)

    def shape(*dims, kind=f32):
        return jax.ShapeDtypeStruct(dims, kind)

    swapped = shifted(jnp.concatenate([given(states, 1), given(x_start, 0)[None]], axis=0), "c", 1)
    states_mine, start_mine = own(states, 1), own(x_start, 0)
    where = jnp.concatenate([jnp.stack([place, group, core]).astype(jnp.int32), own(view_ids, 1)])
    coefs = jnp.stack(coefficients(timesteps))
    size = width // HEADS
    column = jnp.arange(width, dtype=jnp.int32)[None, :]
    head = jnp.arange(HEADS, dtype=jnp.int32)[:, None]
    mask = ((column >= head * size) & (column < (head + 1) * size)).astype(bf16)

    x_shape = shape(steps, rows, width)
    half = shape(steps, part, width)
    places = lax.axis_size(SHARES)
    piece = shape(rows, width, kind=bf16)
    x, start, *mods = call(
        enter_body,
        [x_shape, shape(rows, width)] + [piece] * steps,
        [SMEM] + [VMEM] * 5,
        where,
        states_mine,
        start_mine,
        swapped,
        step_mod,
        view_mod,
    )
    drawn, _ = lax.optimization_barrier((noise, mods[0]))
    noise_mine, noise_peer = own(drawn, 1), shifted(given(drawn, 1), "c", 1)
    for sweep in range(SWEEPS):
        arrived = spread(mods[1:], "x")
        first = call(first_body, shape(rows, 3 * width, kind=bf16), [VMEM] * 2, mods[0], w_qkv)
        *attended, qkv = call(
            others_body,
            [piece] * (steps - 1) + [shape(steps * rows, 3 * width, kind=bf16)],
            [VMEM] * 6,
            first,
            *arrived,
            w_qkv,
            mask,
            scratch=[pltpu.VMEM(((steps - 1) * rows, width), bf16)],
        )
        back = spread(attended, "x", -1)
        kept = call(own_body, piece, [VMEM] * 3, first, qkv, mask)
        base = call(base_body, x_shape, [SMEM] + [VMEM] * 3, coefs, x, noise_mine, noise_peer)
        mine_before, peer_before, total = call(
            project_body,
            [half, half, shape(places, rows // places, width)],
            [SMEM] * 2 + [VMEM] * 8,
            where,
            coefs,
            kept,
            *back,
            w_out,
            base,
            step_mod,
            view_mod,
            scratch=[pltpu.VMEM((steps * rows, width), bf16), pltpu.VMEM((steps * rows, width), f32)],
        )
        if sweep + 1 == SWEEPS:
            break
        lower, _ = earlier_sum(where, total)
        x, *mods = call(
            resume_body,
            [x_shape] + [piece] * steps,
            [SMEM] + [VMEM] * 6,
            where,
            start,
            mine_before,
            peer_before,
            lower,
            step_mod,
            view_mod,
            scratch=[pltpu.VMEM((rows, width), f32)],
        )
    lower, peer_before = earlier_sum(where, total, peer_before)
    return call(
        finish_body,
        shape(*states.shape),
        [SMEM] + [VMEM] * 5,
        where,
        x_start,
        mine_before,
        peer_before,
        lower,
        shifted(lower, "c", 1),
        scratch=[
            pltpu.VMEM((part, width), f32),
            pltpu.VMEM((views, steps, part, width), f32),
            pltpu.SemaphoreType.DMA((views, steps)),
        ],
        out_spec=pl.BlockSpec(memory_space=pl.ANY),
    )


def solution(mesh):
    finer = Mesh(mesh.devices.reshape(2, 2, 2, 4, 4, 2), ("w", "v", "u", "y", "x", "c"))
    tm, tok = ("w", "v", "u", "y"), ("x", "c")
    placed = (
        P(tm, None, tok, None),
        P(tm, None, tok, None),
        P(None, tok, None),
        P(tm),
        P(tm, None, None),
        P(),
        P(tm, None),
        P(),
        P(),
    )
    return jax.shard_map(
        device_program, mesh=finer, in_specs=placed, out_specs=P(tm, None, tok, None), check_vma=False
    )
```

```python
import jax
import jax.numpy as jnp
from jax import lax
from jax.experimental import pallas as pl
from jax.experimental.pallas import tpu as pltpu
from jax.sharding import Mesh
from jax.sharding import PartitionSpec as P


HEADS = 16
SWEEPS = 2
LANES = 128
LOG2E = 1.4426950408889634
SHARES = ("u", "y")
PLANES = ("w", "v", "u")
VMEM = pl.BlockSpec(memory_space=pltpu.VMEM)
SMEM = pl.BlockSpec(memory_space=pltpu.SMEM)


def shifted(value, axis, shift):
    size = lax.axis_size(axis)
    return lax.ppermute(value, axis, [(i, (i + shift) % size) for i in range(size)])


def spread(values, axis, sign=1):
    moved = []
    for k, value in enumerate(values, 1):
        moved.append(shifted(value, axis, sign * k))
    return moved


def call(body, outs, specs, *args, scratch=(), out_spec=VMEM):
    return pl.pallas_call(
        body,
        out_shape=outs,
        in_specs=specs,
        out_specs=jax.tree.map(lambda _: out_spec, outs),
        scratch_shapes=list(scratch),
        compiler_params=pltpu.CompilerParams(vmem_limit_bytes=16 * 2**20),
    )(*args)


def normed_rows(rows, shift, scale):
    center = jnp.mean(rows, axis=-1, keepdims=True)
    off = rows - center
    spread = jnp.mean(off * off, axis=-1, keepdims=True)
    normed = off / jnp.sqrt(spread + 1e-06)
    return (normed * (1.0 + scale) + shift).astype(jnp.bfloat16)


def modulation_row(where_ref, step_ref, view_ref, step, part):
    return step_ref[step, part : part + 1, :] + view_ref[where_ref[4 + step], part : part + 1, :]


def enter_body(where_ref, mine_ref, start_mine, peer_ref, step_ref, view_ref, x_ref, start_ref, *mod_refs):
    place = where_ref[0]
    start_ref[...] = jnp.concatenate([start_mine[...], peer_ref[mine_ref.shape[0]]], axis=0)
    steps = mine_ref.shape[0]
    for r in range(steps):
        step = lax.rem(place + r, steps)
        shift = modulation_row(where_ref, step_ref, view_ref, step, 0)
        scale = modulation_row(where_ref, step_ref, view_ref, step, 1)
        rows = jnp.concatenate([mine_ref[step], peer_ref[step]], axis=0)
        x_ref[step] = rows
        mod_refs[r][...] = normed_rows(rows, shift, scale)


def share_place(flip, q, places):
    half = places // 2
    return (q // half + flip * (1 - 2 * (q // half))) * half + q % half


def resume_body(
    where_ref, start_ref, mine_before, peer_before, lower_ref, step_ref, view_ref, x_ref, *rest
):
    mod_refs, base_ref = rest[:-1], rest[-1]
    place, flip = where_ref[0], where_ref[1]
    steps = mine_before.shape[0]
    places, share, _ = lower_ref.shape
    for q in range(places):
        base_ref[q * share : (q + 1) * share, :] = lower_ref[share_place(flip, q, places)]
    for r in range(steps):
        step = lax.rem(place + r, steps)
        before = jnp.concatenate([mine_before[step], peer_before[step]], axis=0)
        rows = start_ref[...] + (base_ref[...] + before)
        x_ref[step] = rows
        shift = modulation_row(where_ref, step_ref, view_ref, step, 0)
        scale = modulation_row(where_ref, step_ref, view_ref, step, 1)
        mod_refs[r][...] = normed_rows(rows, shift, scale)


def finish_body(
    where_ref, start_ref, mine_before, peer_before, mine_lower, peer_lower, out_ref, base_ref, rows_ref, sems
):
    flip, core = where_ref[1], where_ref[2]
    places, share, _ = mine_lower.shape
    half = places // 2
    sides = ((core, 0, mine_before, mine_lower), (1 - core, half, peer_before, peer_lower))
    copies = []
    for side, (view, low, before_ref, lower_ref) in enumerate(sides):
        for q in range(half):
            rows = slice(q * share, (q + 1) * share)
            base_ref[rows, :] = lower_ref[share_place(flip, low + q, places)]
        for step in range(before_ref.shape[0]):
            rows_ref[side, step] = start_ref[view] + (base_ref[...] + before_ref[step])
            copies.append(
                pltpu.make_async_copy(rows_ref.at[side, step], out_ref.at[step, view], sems.at[side, step])
            )
            copies[-1].start()
    for copy in copies:
        copy.wait()


def project_rows(rows, w_ref):
    return jnp.dot(rows, w_ref[...], preferred_element_type=jnp.float32).astype(jnp.bfloat16)


def first_body(a0, w_ref, qkv_ref):
    qkv_ref[...] = project_rows(a0[...], w_ref)


def attend(q_ref, kv_ref, mask_ref, outs):
    width = mask_ref.shape[1]
    part = outs[0].shape[0]
    size = width // HEADS
    tiles = [None] * (width // LANES)
    for h in range(HEADS):
        first = h * size // LANES
        last = ((h + 1) * size - 1) // LANES
        low, high = first * LANES, (last + 1) * LANES
        q = q_ref[:, low:high] * mask_ref[h : h + 1, low:high]
        k = kv_ref[:, width + low : width + high]
        v = kv_ref[:, 2 * width + low : 2 * width + high]
        scores = lax.dot_general(q, k, (((1,), (1,)), ((), ())), preferred_element_type=jnp.float32)
        top = jnp.max(scores, axis=-1, keepdims=True)
        powers = jnp.exp2((scores - top) * (LOG2E / size**0.5))
        share = 1.0 / jnp.sum(powers, axis=-1, keepdims=True)
        out = jnp.dot(powers.astype(jnp.bfloat16), v, preferred_element_type=jnp.float32) * share
        for t in range(first, last + 1):
            piece = out[:, t * LANES - low : (t + 1) * LANES - low]
            if tiles[t] is not None:
                lane = lax.broadcasted_iota(jnp.int32, piece.shape, 1) + t * LANES
                piece = jnp.where(lane >= h * size, piece, tiles[t])
            tiles[t] = piece
    for t, tile in enumerate(tiles):
        tile = tile.astype(jnp.bfloat16)
        for r, out in enumerate(outs):
            out[:, t * LANES : (t + 1) * LANES] = tile[r * part : (r + 1) * part]


def others_body(first_ref, a1, a2, a3, w_ref, mask_ref, o1, o2, o3, qkv_ref, rows_ref):
    part = a1.shape[0]
    for r, piece in enumerate((a1, a2, a3)):
        rows_ref[r * part : (r + 1) * part, :] = piece[...]
    qkv_ref[: 3 * part, :] = project_rows(rows_ref[...], w_ref)
    qkv_ref[3 * part :, :] = first_ref[...]
    attend(qkv_ref.at[: 3 * part], qkv_ref, mask_ref, (o1, o2, o3))


def own_body(first_ref, qkv_ref, mask_ref, o0):
    attend(first_ref, qkv_ref, mask_ref, (o0,))


def base_body(coef_ref, x_ref, mine_ref, peer_ref, base_ref):
    for step in range(x_ref.shape[0]):
        rows = x_ref[step]
        drawn = jnp.concatenate([mine_ref[step], peer_ref[step]], axis=0).astype(jnp.float32)
        base_ref[step] = (coef_ref[0, step] + coef_ref[1, step]) * rows + coef_ref[2, step] * drawn


def project_body(
    where_ref,
    coef_ref,
    a0,
    a1,
    a2,
    a3,
    w_ref,
    base_ref,
    step_ref,
    view_ref,
    mine_before,
    peer_before,
    total_ref,
    rows_ref,
    proj_ref,
):
    place, flip = where_ref[0], where_ref[1]
    pieces = (a0, a1, a2, a3)
    part = a0.shape[0]
    half = part // 2
    steps = len(pieces)
    for r in range(steps):
        rows = pl.ds(pl.multiple_of(lax.rem(place + r, steps) * part, part), part)
        rows_ref[rows, :] = pieces[r][...]
    proj_ref[...] = jnp.dot(rows_ref[...], w_ref[...], preferred_element_type=jnp.float32)
    running = jnp.zeros((part, proj_ref.shape[1]), jnp.float32)
    for step in range(steps):
        gate = modulation_row(where_ref, step_ref, view_ref, step, 2) * coef_ref[1, step]
        mine_before[step] = running[:half]
        peer_before[step] = running[half:]
        running = running + (base_ref[step] + gate * proj_ref[step * part : (step + 1) * part, :])
    places, share, _ = total_ref.shape
    for q in range(places):
        total_ref[share_place(flip, q, places)] = running[q * share : (q + 1) * share]


def coefficients(steps_index):
    unit = steps_index.astype(jnp.float32) / 1000.0
    beta = 0.1 + 19.9 * unit
    sigma = jnp.sqrt(1.0 - jnp.exp(-(0.1 * unit + 9.95 * unit * unit)))
    coef_state = 0.5 * beta * 0.004
    coef_eps = beta * 0.004 / sigma
    coef_noise = jnp.sqrt(beta * 0.004)
    return (coef_state, coef_eps, coef_noise)


def inside_body(held_ref, before_ref, all_ref):
    running = jnp.zeros(held_ref.shape[1:], held_ref.dtype)
    for q in range(held_ref.shape[0]):
        before_ref[q] = running
        running = running + held_ref[q]
    all_ref[...] = running


def below_body(where_ref, before_ref, near_ref, far_ref, out_ref):
    below = jnp.where(where_ref[3] == 1, near_ref[...], 0.0) + jnp.where(where_ref[1] == 1, far_ref[...], 0.0)
    for q in range(before_ref.shape[0]):
        out_ref[q] = before_ref[q] + below


def earlier_sum(where, shares, beside=None):
    held = lax.all_to_all(shares, SHARES, 0, 0, tiled=True)
    whole = jax.ShapeDtypeStruct(shares.shape, shares.dtype)
    before, total = call(inside_body, [whole, jax.ShapeDtypeStruct(shares.shape[1:], shares.dtype)], [VMEM], held)
    near = shifted(total, "v", 1)
    planes = lax.axis_size(PLANES)
    far = lax.ppermute(total + near, PLANES, [(i, planes - 1 - i) for i in range(planes)])
    if beside is not None:
        far, beside = lax.optimization_barrier((far, shifted(beside, "c", 1)))
    sums = call(below_body, whole, [SMEM] + [VMEM] * 3, where, before, near, far)
    return lax.all_to_all(sums, SHARES, 0, 0, tiled=True), beside


def device_program(states, noise, x_start, timesteps, step_mod, view_mod, view_ids, w_qkv, w_out):
    steps, views, part, width = states.shape
    place, flip, core, odd = (lax.axis_index(a) for a in ("x", "w", "c", "v"))
    other = 1 - core
    f32, bf16 = jnp.float32, jnp.bfloat16
    rows = 2 * part

    def own(a, axis):
        return lax.dynamic_index_in_dim(a, core, axis, keepdims=False)

    def given(a, axis):
        return lax.dynamic_index_in_dim(a, other, axis, keepdims=False)

    def shape(*dims, kind=f32):
        return jax.ShapeDtypeStruct(dims, kind)

    swapped = shifted(jnp.concatenate([given(states, 1), given(x_start, 0)[None]], axis=0), "c", 1)
    states_mine, start_mine = own(states, 1), own(x_start, 0)
    where = jnp.concatenate([jnp.stack([place, flip, core, odd]).astype(jnp.int32), own(view_ids, 1)])
    coefs = jnp.stack(coefficients(timesteps))
    size = width // HEADS
    column = jnp.arange(width, dtype=jnp.int32)[None, :]
    head = jnp.arange(HEADS, dtype=jnp.int32)[:, None]
    mask = ((column >= head * size) & (column < (head + 1) * size)).astype(bf16)

    x_shape = shape(steps, rows, width)
    half = shape(steps, part, width)
    places = lax.axis_size(SHARES)
    piece = shape(rows, width, kind=bf16)
    x, start, *mods = call(
        enter_body,
        [x_shape, shape(rows, width)] + [piece] * steps,
        [SMEM] + [VMEM] * 5,
        where,
        states_mine,
        start_mine,
        swapped,
        step_mod,
        view_mod,
    )
    drawn, _ = lax.optimization_barrier((noise, mods[0]))
    noise_mine, noise_peer = own(drawn, 1), shifted(given(drawn, 1), "c", 1)
    for sweep in range(SWEEPS):
        arrived = spread(mods[1:], "x")
        first = call(first_body, shape(rows, 3 * width, kind=bf16), [VMEM] * 2, mods[0], w_qkv)
        *attended, qkv = call(
            others_body,
            [piece] * (steps - 1) + [shape(steps * rows, 3 * width, kind=bf16)],
            [VMEM] * 6,
            first,
            *arrived,
            w_qkv,
            mask,
            scratch=[pltpu.VMEM(((steps - 1) * rows, width), bf16)],
        )
        back = spread(attended, "x", -1)
        kept = call(own_body, piece, [VMEM] * 3, first, qkv, mask)
        base = call(base_body, x_shape, [SMEM] + [VMEM] * 3, coefs, x, noise_mine, noise_peer)
        mine_before, peer_before, total = call(
            project_body,
            [half, half, shape(places, rows // places, width)],
            [SMEM] * 2 + [VMEM] * 8,
            where,
            coefs,
            kept,
            *back,
            w_out,
            base,
            step_mod,
            view_mod,
            scratch=[pltpu.VMEM((steps * rows, width), bf16), pltpu.VMEM((steps * rows, width), f32)],
        )
        if sweep + 1 == SWEEPS:
            break
        lower, _ = earlier_sum(where, total)
        x, *mods = call(
            resume_body,
            [x_shape] + [piece] * steps,
            [SMEM] + [VMEM] * 6,
            where,
            start,
            mine_before,
            peer_before,
            lower,
            step_mod,
            view_mod,
            scratch=[pltpu.VMEM((rows, width), f32)],
        )
    lower, peer_before = earlier_sum(where, total, peer_before)
    return call(
        finish_body,
        shape(*states.shape),
        [SMEM] + [VMEM] * 5,
        where,
        x_start,
        mine_before,
        peer_before,
        lower,
        shifted(lower, "c", 1),
        scratch=[
            pltpu.VMEM((part, width), f32),
            pltpu.VMEM((views, steps, part, width), f32),
            pltpu.SemaphoreType.DMA((views, steps)),
        ],
        out_spec=pl.BlockSpec(memory_space=pl.ANY),
    )


def solution(mesh):
    finer = Mesh(mesh.devices.reshape(2, 2, 2, 4, 4, 2), ("w", "v", "u", "y", "x", "c"))
    tm, tok = ("w", "v", "u", "y"), ("x", "c")
    placed = (
        P(tm, None, tok, None),
        P(tm, None, tok, None),
        P(None, tok, None),
        P(tm),
        P(tm, None, None),
        P(),
        P(tm, None),
        P(),
        P(),
    )
    return jax.shard_map(device_program, mesh=finer, in_specs=placed, out_specs=P(tm, None, tok, None), check_vma=False)
```

```python
import jax
import jax.numpy as jnp
from jax import lax
from jax.experimental import pallas as pl
from jax.experimental.pallas import tpu as pltpu
from jax.sharding import Mesh
from jax.sharding import PartitionSpec as P


HEADS = 16
HEAD_BATCH = 8
SWEEPS = 2
LANES = 128
LOG2E = 1.4426950408889634
SHARES = ("u", "y")
GROUPS = ("w", "v")
VMEM = pl.BlockSpec(memory_space=pltpu.VMEM)
SMEM = pl.BlockSpec(memory_space=pltpu.SMEM)


def shifted(value, axis, shift):
    size = lax.axis_size(axis)
    return lax.ppermute(value, axis, [(i, (i + shift) % size) for i in range(size)])


def spread(values, axis, sign=1):
    moved = []
    for k, value in enumerate(values, 1):
        moved.append(shifted(value, axis, sign * k))
    return moved


def call(body, outs, specs, *args, scratch=(), out_spec=VMEM):
    return pl.pallas_call(
        body,
        out_shape=outs,
        in_specs=specs,
        out_specs=jax.tree.map(lambda _: out_spec, outs),
        scratch_shapes=list(scratch),
        compiler_params=pltpu.CompilerParams(vmem_limit_bytes=16 * 2**20),
    )(*args)


def normed_rows(rows, shift, scale):
    center = jnp.mean(rows, axis=-1, keepdims=True)
    off = rows - center
    spread = jnp.mean(off * off, axis=-1, keepdims=True)
    normed = off / jnp.sqrt(spread + 1e-06)
    return (normed * (1.0 + scale) + shift).astype(jnp.bfloat16)


def modulation_row(where_ref, step_ref, view_ref, step, part):
    return step_ref[step, part : part + 1, :] + view_ref[where_ref[3 + step], part : part + 1, :]


def enter_body(where_ref, mine_ref, start_mine, peer_ref, step_ref, view_ref, x_ref, start_ref, *mod_refs):
    place = where_ref[0]
    start_ref[...] = jnp.concatenate([start_mine[...], peer_ref[mine_ref.shape[0]]], axis=0)
    steps = mine_ref.shape[0]
    for r in range(steps):
        step = lax.rem(place + r, steps)
        shift = modulation_row(where_ref, step_ref, view_ref, step, 0)
        scale = modulation_row(where_ref, step_ref, view_ref, step, 1)
        rows = jnp.concatenate([mine_ref[step], peer_ref[step]], axis=0)
        x_ref[step] = rows
        mod_refs[r][...] = normed_rows(rows, shift, scale)


def resume_body(
    where_ref, start_ref, mine_before, peer_before, lower_ref, step_ref, view_ref, x_ref, *rest
):
    mod_refs, base_ref = rest[:-1], rest[-1]
    place = where_ref[0]
    steps = mine_before.shape[0]
    places, share, _ = lower_ref.shape
    for q in range(places):
        base_ref[q * share : (q + 1) * share, :] = lower_ref[q]
    for r in range(steps):
        step = lax.rem(place + r, steps)
        before = jnp.concatenate([mine_before[step], peer_before[step]], axis=0)
        rows = start_ref[...] + (base_ref[...] + before)
        x_ref[step] = rows
        shift = modulation_row(where_ref, step_ref, view_ref, step, 0)
        scale = modulation_row(where_ref, step_ref, view_ref, step, 1)
        mod_refs[r][...] = normed_rows(rows, shift, scale)


def finish_body(
    where_ref, start_ref, mine_before, peer_before, mine_lower, peer_lower, out_ref, base_ref, rows_ref, sems
):
    core = where_ref[2]
    places, share, _ = mine_lower.shape
    half = places // 2
    sides = ((core, 0, mine_before, mine_lower), (1 - core, half, peer_before, peer_lower))
    copies = []
    for side, (view, low, before_ref, lower_ref) in enumerate(sides):
        for q in range(half):
            rows = slice(q * share, (q + 1) * share)
            base_ref[rows, :] = lower_ref[low + q]
        for step in range(before_ref.shape[0]):
            rows_ref[side, step] = start_ref[view] + (base_ref[...] + before_ref[step])
            copies.append(
                pltpu.make_async_copy(rows_ref.at[side, step], out_ref.at[step, view], sems.at[side, step])
            )
            copies[-1].start()
    for copy in copies:
        copy.wait()


def project_rows(rows, w_ref):
    return jnp.dot(rows, w_ref[...], preferred_element_type=jnp.float32).astype(jnp.bfloat16)


def first_body(a0, w_ref, qkv_ref):
    qkv_ref[...] = project_rows(a0[...], w_ref)


def attend(q_ref, kv_ref, mask_ref, outs, scores_ref, probs_ref):
    width = mask_ref.shape[1]
    part = outs[0].shape[0]
    size = width // HEADS
    batch = scores_ref.shape[0]
    tiles = [None] * (width // LANES)

    def window(h):
        first = h * size // LANES
        last = ((h + 1) * size - 1) // LANES
        return first, last, first * LANES, (last + 1) * LANES

    for start in range(0, HEADS, batch):
        heads = range(start, start + batch)
        shares = []
        for h in heads:
            _, _, low, high = window(h)
            q = q_ref[:, low:high] * mask_ref[h : h + 1, low:high]
            k = kv_ref[:, width + low : width + high]
            scores_ref[h - start] = lax.dot_general(
                q, k, (((1,), (1,)), ((), ())), preferred_element_type=jnp.float32
            )
        for h in heads:
            scores = scores_ref[h - start]
            top = jnp.max(scores, axis=-1, keepdims=True)
            powers = jnp.exp2((scores - top) * (LOG2E / size**0.5))
            shares.append(1.0 / jnp.sum(powers, axis=-1, keepdims=True))
            probs_ref[h - start] = powers.astype(jnp.bfloat16)
        for h in heads:
            first, last, low, high = window(h)
            v = kv_ref[:, 2 * width + low : 2 * width + high]
            out = jnp.dot(probs_ref[h - start], v, preferred_element_type=jnp.float32) * shares[h - start]
            for t in range(first, last + 1):
                piece = out[:, t * LANES - low : (t + 1) * LANES - low]
                if tiles[t] is not None:
                    lane = lax.broadcasted_iota(jnp.int32, piece.shape, 1) + t * LANES
                    piece = jnp.where(lane >= h * size, piece, tiles[t])
                tiles[t] = piece
                if (t + 1) * LANES <= (h + 1) * size:
                    tile = piece.astype(jnp.bfloat16)
                    for r, out_ref in enumerate(outs):
                        out_ref[:, t * LANES : (t + 1) * LANES] = tile[r * part : (r + 1) * part]


def stages(queries, keys):
    return [
        pltpu.VMEM((HEAD_BATCH, queries, keys), jnp.float32),
        pltpu.VMEM((HEAD_BATCH, queries, keys), jnp.bfloat16),
    ]


def others_body(
    first_ref, a1, a2, a3, w_ref, mask_ref, o1, o2, o3, qkv_ref, rows_ref, scores_ref, probs_ref
):
    part = a1.shape[0]
    for r, piece in enumerate((a1, a2, a3)):
        rows_ref[r * part : (r + 1) * part, :] = piece[...]
    qkv_ref[: 3 * part, :] = project_rows(rows_ref[...], w_ref)
    qkv_ref[3 * part :, :] = first_ref[...]
    attend(qkv_ref.at[: 3 * part], qkv_ref, mask_ref, (o1, o2, o3), scores_ref, probs_ref)


def own_body(first_ref, qkv_ref, mask_ref, o0, scores_ref, probs_ref):
    attend(first_ref, qkv_ref, mask_ref, (o0,), scores_ref, probs_ref)


def base_body(coef_ref, x_ref, mine_ref, peer_ref, base_ref):
    for step in range(x_ref.shape[0]):
        rows = x_ref[step]
        drawn = jnp.concatenate([mine_ref[step], peer_ref[step]], axis=0).astype(jnp.float32)
        base_ref[step] = (coef_ref[0, step] + coef_ref[1, step]) * rows + coef_ref[2, step] * drawn


def project_body(
    where_ref,
    coef_ref,
    a0,
    a1,
    a2,
    a3,
    w_ref,
    base_ref,
    step_ref,
    view_ref,
    mine_before,
    peer_before,
    total_ref,
    rows_ref,
    proj_ref,
):
    place = where_ref[0]
    pieces = (a0, a1, a2, a3)
    part = a0.shape[0]
    half = part // 2
    steps = len(pieces)
    for r in range(steps):
        rows = pl.ds(pl.multiple_of(lax.rem(place + r, steps) * part, part), part)
        rows_ref[rows, :] = pieces[r][...]
    proj_ref[...] = jnp.dot(rows_ref[...], w_ref[...], preferred_element_type=jnp.float32)
    running = jnp.zeros((part, proj_ref.shape[1]), jnp.float32)
    for step in range(steps):
        gate = modulation_row(where_ref, step_ref, view_ref, step, 2) * coef_ref[1, step]
        mine_before[step] = running[:half]
        peer_before[step] = running[half:]
        running = running + (base_ref[step] + gate * proj_ref[step * part : (step + 1) * part, :])
    places, share, _ = total_ref.shape
    for q in range(places):
        total_ref[q] = running[q * share : (q + 1) * share]


def coefficients(steps_index):
    unit = steps_index.astype(jnp.float32) / 1000.0
    beta = 0.1 + 19.9 * unit
    sigma = jnp.sqrt(1.0 - jnp.exp(-(0.1 * unit + 9.95 * unit * unit)))
    coef_state = 0.5 * beta * 0.004
    coef_eps = beta * 0.004 / sigma
    coef_noise = jnp.sqrt(beta * 0.004)
    return (coef_state, coef_eps, coef_noise)


def inside_body(held_ref, before_ref, all_ref):
    running = jnp.zeros(held_ref.shape[1:], held_ref.dtype)
    for q in range(held_ref.shape[0]):
        before_ref[q] = running
        running = running + held_ref[q]
    all_ref[...] = running


def below_body(where_ref, before_ref, *refs):
    passed, out_ref = refs[:-1], refs[-1]
    group = where_ref[1]
    below = jnp.zeros(before_ref.shape[1:], before_ref.dtype)
    for shift, ref in enumerate(passed, 1):
        below = below + jnp.where(shift <= group, ref[...], 0.0)
    for q in range(before_ref.shape[0]):
        out_ref[q] = before_ref[q] + below


def earlier_sum(where, shares, beside=None):
    held = lax.all_to_all(shares, SHARES, 0, 0, tiled=True)
    whole = jax.ShapeDtypeStruct(shares.shape, shares.dtype)
    before, total = call(inside_body, [whole, jax.ShapeDtypeStruct(shares.shape[1:], shares.dtype)], [VMEM], held)
    passed = spread([total] * (lax.axis_size(GROUPS) - 1), GROUPS)
    if beside is not None:
        passed[0], beside = lax.optimization_barrier((passed[0], shifted(beside, "c", 1)))
    sums = call(below_body, whole, [SMEM] + [VMEM] * (1 + len(passed)), where, before, *passed)
    return lax.all_to_all(sums, SHARES, 0, 0, tiled=True), beside


def device_program(states, noise, x_start, timesteps, step_mod, view_mod, view_ids, w_qkv, w_out):
    steps, views, part, width = states.shape
    place, group, core = (lax.axis_index(a) for a in ("x", GROUPS, "c"))
    other = 1 - core
    f32, bf16 = jnp.float32, jnp.bfloat16
    rows = 2 * part

    def own(a, axis):
        return lax.dynamic_index_in_dim(a, core, axis, keepdims=False)

    def given(a, axis):
        return lax.dynamic_index_in_dim(a, other, axis, keepdims=False)

    def shape(*dims, kind=f32):
        return jax.ShapeDtypeStruct(dims, kind)

    swapped = shifted(jnp.concatenate([given(states, 1), given(x_start, 0)[None]], axis=0), "c", 1)
    states_mine, start_mine = own(states, 1), own(x_start, 0)
    where = jnp.concatenate([jnp.stack([place, group, core]).astype(jnp.int32), own(view_ids, 1)])
    coefs = jnp.stack(coefficients(timesteps))
    size = width // HEADS
    column = jnp.arange(width, dtype=jnp.int32)[None, :]
    head = jnp.arange(HEADS, dtype=jnp.int32)[:, None]
    mask = ((column >= head * size) & (column < (head + 1) * size)).astype(bf16)

    x_shape = shape(steps, rows, width)
    half = shape(steps, part, width)
    places = lax.axis_size(SHARES)
    piece = shape(rows, width, kind=bf16)
    x, start, *mods = call(
        enter_body,
        [x_shape, shape(rows, width)] + [piece] * steps,
        [SMEM] + [VMEM] * 5,
        where,
        states_mine,
        start_mine,
        swapped,
        step_mod,
        view_mod,
    )
    drawn, _ = lax.optimization_barrier((noise, mods[0]))
    noise_mine, noise_peer = own(drawn, 1), shifted(given(drawn, 1), "c", 1)
    for sweep in range(SWEEPS):
        arrived = spread(mods[1:], "x")
        first = call(first_body, shape(rows, 3 * width, kind=bf16), [VMEM] * 2, mods[0], w_qkv)
        *attended, qkv = call(
            others_body,
            [piece] * (steps - 1) + [shape(steps * rows, 3 * width, kind=bf16)],
            [VMEM] * 6,
            first,
            *arrived,
            w_qkv,
            mask,
            scratch=[pltpu.VMEM(((steps - 1) * rows, width), bf16)] + stages((steps - 1) * rows, steps * rows),
        )
        back = spread(attended, "x", -1)
        kept = call(
            own_body, piece, [VMEM] * 3, first, qkv, mask, scratch=stages(rows, steps * rows)
        )
        base = call(base_body, x_shape, [SMEM] + [VMEM] * 3, coefs, x, noise_mine, noise_peer)
        mine_before, peer_before, total = call(
            project_body,
            [half, half, shape(places, rows // places, width)],
            [SMEM] * 2 + [VMEM] * 8,
            where,
            coefs,
            kept,
            *back,
            w_out,
            base,
            step_mod,
            view_mod,
            scratch=[pltpu.VMEM((steps * rows, width), bf16), pltpu.VMEM((steps * rows, width), f32)],
        )
        if sweep + 1 == SWEEPS:
            break
        lower, _ = earlier_sum(where, total)
        x, *mods = call(
            resume_body,
            [x_shape] + [piece] * steps,
            [SMEM] + [VMEM] * 6,
            where,
            start,
            mine_before,
            peer_before,
            lower,
            step_mod,
            view_mod,
            scratch=[pltpu.VMEM((rows, width), f32)],
        )
    lower, peer_before = earlier_sum(where, total, peer_before)
    return call(
        finish_body,
        shape(*states.shape),
        [SMEM] + [VMEM] * 5,
        where,
        x_start,
        mine_before,
        peer_before,
        lower,
        shifted(lower, "c", 1),
        scratch=[
            pltpu.VMEM((part, width), f32),
            pltpu.VMEM((views, steps, part, width), f32),
            pltpu.SemaphoreType.DMA((views, steps)),
        ],
        out_spec=pl.BlockSpec(memory_space=pl.ANY),
    )


def solution(mesh):
    finer = Mesh(mesh.devices.reshape(2, 2, 2, 4, 4, 2), ("w", "v", "u", "y", "x", "c"))
    tm, tok = ("w", "v", "u", "y"), ("x", "c")
    placed = (
        P(tm, None, tok, None),
        P(tm, None, tok, None),
        P(None, tok, None),
        P(tm),
        P(tm, None, None),
        P(),
        P(tm, None),
        P(),
        P(),
    )
    return jax.shard_map(device_program, mesh=finer, in_specs=placed, out_specs=P(tm, None, tok, None), check_vma=False)
```

```python
import jax
import jax.numpy as jnp
from jax import lax
from jax.experimental import pallas as pl
from jax.experimental.pallas import tpu as pltpu
from jax.sharding import Mesh
from jax.sharding import PartitionSpec as P


HEADS = 16
HEAD_BATCH = 8
SWEEPS = 2
LANES = 128
LOG2E = 1.4426950408889634
SHARES = ("u", "y")
GROUPS = ("w", "v")
VMEM = pl.BlockSpec(memory_space=pltpu.VMEM)
SMEM = pl.BlockSpec(memory_space=pltpu.SMEM)


def shifted(value, axis, shift):
    size = lax.axis_size(axis)
    return lax.ppermute(value, axis, [(i, (i + shift) % size) for i in range(size)])


def spread(values, axis, sign=1):
    moved = []
    for k, value in enumerate(values, 1):
        moved.append(shifted(value, axis, sign * k))
    return moved


def call(body, outs, specs, *args, scratch=(), out_spec=VMEM):
    return pl.pallas_call(
        body,
        out_shape=outs,
        in_specs=specs,
        out_specs=jax.tree.map(lambda _: out_spec, outs),
        scratch_shapes=list(scratch),
        compiler_params=pltpu.CompilerParams(vmem_limit_bytes=16 * 2**20),
    )(*args)


def normed_rows(rows, shift, scale):
    center = jnp.mean(rows, axis=-1, keepdims=True)
    off = rows - center
    spread = jnp.mean(off * off, axis=-1, keepdims=True)
    normed = off / jnp.sqrt(spread + 1e-06)
    return (normed * (1.0 + scale) + shift).astype(jnp.bfloat16)


def modulation_row(where_ref, step_ref, view_ref, step, part):
    return step_ref[step, part : part + 1, :] + view_ref[where_ref[3 + step], part : part + 1, :]


def give_body(core_ref, states_ref, start_ref, out_ref):
    other = 1 - core_ref[0]
    steps = states_ref.shape[0]
    for step in range(steps):
        out_ref[step] = states_ref[step, other]
    out_ref[steps] = start_ref[other]


def enter_body(where_ref, states_ref, all_start, peer_ref, step_ref, view_ref, x_ref, start_ref, *mod_refs):
    place, core = where_ref[0], where_ref[2]
    steps = states_ref.shape[0]
    start_ref[...] = jnp.concatenate([all_start[core], peer_ref[steps]], axis=0)
    for r in range(steps):
        step = lax.rem(place + r, steps)
        shift = modulation_row(where_ref, step_ref, view_ref, step, 0)
        scale = modulation_row(where_ref, step_ref, view_ref, step, 1)
        rows = jnp.concatenate([states_ref[step, core], peer_ref[step]], axis=0)
        x_ref[step] = rows
        mod_refs[r][...] = normed_rows(rows, shift, scale)


def resume_body(
    where_ref, start_ref, mine_before, peer_before, lower_ref, step_ref, view_ref, x_ref, *rest
):
    mod_refs, base_ref = rest[:-1], rest[-1]
    place = where_ref[0]
    steps = mine_before.shape[0]
    places, share, _ = lower_ref.shape
    for q in range(places):
        base_ref[q * share : (q + 1) * share, :] = lower_ref[q]
    for r in range(steps):
        step = lax.rem(place + r, steps)
        before = jnp.concatenate([mine_before[step], peer_before[step]], axis=0)
        rows = start_ref[...] + (base_ref[...] + before)
        x_ref[step] = rows
        shift = modulation_row(where_ref, step_ref, view_ref, step, 0)
        scale = modulation_row(where_ref, step_ref, view_ref, step, 1)
        mod_refs[r][...] = normed_rows(rows, shift, scale)


def finish_body(
    where_ref, start_ref, mine_before, peer_before, mine_lower, peer_lower, out_ref, base_ref, rows_ref, sems
):
    core = where_ref[2]
    places, share, _ = mine_lower.shape
    half = places // 2
    sides = ((core, 0, mine_before, mine_lower), (1 - core, half, peer_before, peer_lower))
    copies = []
    for side, (view, low, before_ref, lower_ref) in enumerate(sides):
        for q in range(half):
            rows = slice(q * share, (q + 1) * share)
            base_ref[rows, :] = lower_ref[low + q]
        for step in range(before_ref.shape[0]):
            rows_ref[side, step] = start_ref[view] + (base_ref[...] + before_ref[step])
            copies.append(
                pltpu.make_async_copy(rows_ref.at[side, step], out_ref.at[step, view], sems.at[side, step])
            )
            copies[-1].start()
    for copy in copies:
        copy.wait()


def project_rows(rows, w_ref):
    return jnp.dot(rows, w_ref[...], preferred_element_type=jnp.float32).astype(jnp.bfloat16)


def first_body(a0, w_ref, qkv_ref):
    qkv_ref[...] = project_rows(a0[...], w_ref)


def attend(q_ref, kv_ref, mask_ref, outs, scores_ref, probs_ref):
    width = mask_ref.shape[1]
    part = outs[0].shape[0]
    size = width // HEADS
    batch = scores_ref.shape[0]
    tiles = [None] * (width // LANES)

    def window(h):
        first = h * size // LANES
        last = ((h + 1) * size - 1) // LANES
        return first, last, first * LANES, (last + 1) * LANES

    for start in range(0, HEADS, batch):
        heads = range(start, start + batch)
        shares = []
        for h in heads:
            _, _, low, high = window(h)
            q = q_ref[:, low:high] * mask_ref[h : h + 1, low:high]
            k = kv_ref[:, width + low : width + high]
            scores_ref[h - start] = lax.dot_general(
                q, k, (((1,), (1,)), ((), ())), preferred_element_type=jnp.float32
            )
        for h in heads:
            scores = scores_ref[h - start]
            top = jnp.max(scores, axis=-1, keepdims=True)
            powers = jnp.exp2((scores - top) * (LOG2E / size**0.5))
            shares.append(1.0 / jnp.sum(powers, axis=-1, keepdims=True))
            probs_ref[h - start] = powers.astype(jnp.bfloat16)
        for h in heads:
            first, last, low, high = window(h)
            v = kv_ref[:, 2 * width + low : 2 * width + high]
            out = jnp.dot(probs_ref[h - start], v, preferred_element_type=jnp.float32) * shares[h - start]
            for t in range(first, last + 1):
                piece = out[:, t * LANES - low : (t + 1) * LANES - low]
                if tiles[t] is not None:
                    lane = lax.broadcasted_iota(jnp.int32, piece.shape, 1) + t * LANES
                    piece = jnp.where(lane >= h * size, piece, tiles[t])
                tiles[t] = piece
                if (t + 1) * LANES <= (h + 1) * size:
                    tile = piece.astype(jnp.bfloat16)
                    for r, out_ref in enumerate(outs):
                        out_ref[:, t * LANES : (t + 1) * LANES] = tile[r * part : (r + 1) * part]


def stages(queries, keys):
    return [
        pltpu.VMEM((HEAD_BATCH, queries, keys), jnp.float32),
        pltpu.VMEM((HEAD_BATCH, queries, keys), jnp.bfloat16),
    ]


def others_body(
    first_ref, a1, a2, a3, w_ref, mask_ref, o1, o2, o3, qkv_ref, rows_ref, scores_ref, probs_ref
):
    part = a1.shape[0]
    for r, piece in enumerate((a1, a2, a3)):
        rows_ref[r * part : (r + 1) * part, :] = piece[...]
    qkv_ref[: 3 * part, :] = project_rows(rows_ref[...], w_ref)
    qkv_ref[3 * part :, :] = first_ref[...]
    attend(qkv_ref.at[: 3 * part], qkv_ref, mask_ref, (o1, o2, o3), scores_ref, probs_ref)


def own_body(first_ref, qkv_ref, mask_ref, o0, scores_ref, probs_ref):
    attend(first_ref, qkv_ref, mask_ref, (o0,), scores_ref, probs_ref)


def base_body(coef_ref, x_ref, mine_ref, peer_ref, base_ref):
    for step in range(x_ref.shape[0]):
        rows = x_ref[step]
        drawn = jnp.concatenate([mine_ref[step], peer_ref[step]], axis=0).astype(jnp.float32)
        base_ref[step] = (coef_ref[0, step] + coef_ref[1, step]) * rows + coef_ref[2, step] * drawn


def project_body(
    where_ref,
    coef_ref,
    a0,
    a1,
    a2,
    a3,
    w_ref,
    base_ref,
    step_ref,
    view_ref,
    mine_before,
    peer_before,
    total_ref,
    rows_ref,
    proj_ref,
):
    place = where_ref[0]
    pieces = (a0, a1, a2, a3)
    part = a0.shape[0]
    half = part // 2
    steps = len(pieces)
    for r in range(steps):
        rows = pl.ds(pl.multiple_of(lax.rem(place + r, steps) * part, part), part)
        rows_ref[rows, :] = pieces[r][...]
    proj_ref[...] = jnp.dot(rows_ref[...], w_ref[...], preferred_element_type=jnp.float32)
    running = jnp.zeros((part, proj_ref.shape[1]), jnp.float32)
    for step in range(steps):
        gate = modulation_row(where_ref, step_ref, view_ref, step, 2) * coef_ref[1, step]
        mine_before[step] = running[:half]
        peer_before[step] = running[half:]
        running = running + (base_ref[step] + gate * proj_ref[step * part : (step + 1) * part, :])
    places, share, _ = total_ref.shape
    for q in range(places):
        total_ref[q] = running[q * share : (q + 1) * share]


def coefficients(steps_index):
    unit = steps_index.astype(jnp.float32) / 1000.0
    beta = 0.1 + 19.9 * unit
    sigma = jnp.sqrt(1.0 - jnp.exp(-(0.1 * unit + 9.95 * unit * unit)))
    coef_state = 0.5 * beta * 0.004
    coef_eps = beta * 0.004 / sigma
    coef_noise = jnp.sqrt(beta * 0.004)
    return (coef_state, coef_eps, coef_noise)


def inside_body(held_ref, before_ref, all_ref):
    running = jnp.zeros(held_ref.shape[1:], held_ref.dtype)
    for q in range(held_ref.shape[0]):
        before_ref[q] = running
        running = running + held_ref[q]
    all_ref[...] = running


def below_body(where_ref, before_ref, *refs):
    passed, out_ref = refs[:-1], refs[-1]
    group = where_ref[1]
    below = jnp.zeros(before_ref.shape[1:], before_ref.dtype)
    for shift, ref in enumerate(passed, 1):
        below = below + jnp.where(shift <= group, ref[...], 0.0)
    for q in range(before_ref.shape[0]):
        out_ref[q] = before_ref[q] + below


def earlier_sum(where, shares, beside=None):
    held = lax.all_to_all(shares, SHARES, 0, 0, tiled=True)
    whole = jax.ShapeDtypeStruct(shares.shape, shares.dtype)
    before, total = call(inside_body, [whole, jax.ShapeDtypeStruct(shares.shape[1:], shares.dtype)], [VMEM], held)
    passed = spread([total] * (lax.axis_size(GROUPS) - 1), GROUPS)
    if beside is not None:
        passed[0], beside = lax.optimization_barrier((passed[0], shifted(beside, "c", 1)))
    sums = call(below_body, whole, [SMEM] + [VMEM] * (1 + len(passed)), where, before, *passed)
    return lax.all_to_all(sums, SHARES, 0, 0, tiled=True), beside


def device_program(states, noise, x_start, timesteps, step_mod, view_mod, view_ids, w_qkv, w_out):
    steps, views, part, width = states.shape
    place, group, core = (lax.axis_index(a) for a in ("x", GROUPS, "c"))
    other = 1 - core
    f32, bf16 = jnp.float32, jnp.bfloat16
    rows = 2 * part

    def own(a, axis):
        return lax.dynamic_index_in_dim(a, core, axis, keepdims=False)

    def given(a, axis):
        return lax.dynamic_index_in_dim(a, other, axis, keepdims=False)

    def shape(*dims, kind=f32):
        return jax.ShapeDtypeStruct(dims, kind)

    cores = jnp.reshape(core, (1,)).astype(jnp.int32)
    given_rows = call(give_body, shape(steps + 1, part, width), [SMEM] + [VMEM] * 2, cores, states, x_start)
    swapped = shifted(given_rows, "c", 1)
    where = jnp.concatenate([jnp.stack([place, group, core]).astype(jnp.int32), own(view_ids, 1)])
    coefs = jnp.stack(coefficients(timesteps))
    size = width // HEADS
    column = jnp.arange(width, dtype=jnp.int32)[None, :]
    head = jnp.arange(HEADS, dtype=jnp.int32)[:, None]
    mask = ((column >= head * size) & (column < (head + 1) * size)).astype(bf16)

    x_shape = shape(steps, rows, width)
    half = shape(steps, part, width)
    places = lax.axis_size(SHARES)
    piece = shape(rows, width, kind=bf16)
    x, start, *mods = call(
        enter_body,
        [x_shape, shape(rows, width)] + [piece] * steps,
        [SMEM] + [VMEM] * 5,
        where,
        states,
        x_start,
        swapped,
        step_mod,
        view_mod,
    )
    drawn, _ = lax.optimization_barrier((noise, mods[0]))
    noise_mine, noise_peer = own(drawn, 1), shifted(given(drawn, 1), "c", 1)
    for sweep in range(SWEEPS):
        arrived = spread(mods[1:], "x")
        first = call(first_body, shape(rows, 3 * width, kind=bf16), [VMEM] * 2, mods[0], w_qkv)
        *attended, qkv = call(
            others_body,
            [piece] * (steps - 1) + [shape(steps * rows, 3 * width, kind=bf16)],
            [VMEM] * 6,
            first,
            *arrived,
            w_qkv,
            mask,
            scratch=[pltpu.VMEM(((steps - 1) * rows, width), bf16)] + stages((steps - 1) * rows, steps * rows),
        )
        back = spread(attended, "x", -1)
        kept = call(
            own_body, piece, [VMEM] * 3, first, qkv, mask, scratch=stages(rows, steps * rows)
        )
        base = call(base_body, x_shape, [SMEM] + [VMEM] * 3, coefs, x, noise_mine, noise_peer)
        mine_before, peer_before, total = call(
            project_body,
            [half, half, shape(places, rows // places, width)],
            [SMEM] * 2 + [VMEM] * 8,
            where,
            coefs,
            kept,
            *back,
            w_out,
            base,
            step_mod,
            view_mod,
            scratch=[pltpu.VMEM((steps * rows, width), bf16), pltpu.VMEM((steps * rows, width), f32)],
        )
        if sweep + 1 == SWEEPS:
            break
        lower, _ = earlier_sum(where, total)
        x, *mods = call(
            resume_body,
            [x_shape] + [piece] * steps,
            [SMEM] + [VMEM] * 6,
            where,
            start,
            mine_before,
            peer_before,
            lower,
            step_mod,
            view_mod,
            scratch=[pltpu.VMEM((rows, width), f32)],
        )
    lower, peer_before = earlier_sum(where, total, peer_before)
    return call(
        finish_body,
        shape(*states.shape),
        [SMEM] + [VMEM] * 5,
        where,
        x_start,
        mine_before,
        peer_before,
        lower,
        shifted(lower, "c", 1),
        scratch=[
            pltpu.VMEM((part, width), f32),
            pltpu.VMEM((views, steps, part, width), f32),
            pltpu.SemaphoreType.DMA((views, steps)),
        ],
        out_spec=pl.BlockSpec(memory_space=pl.ANY),
    )


def solution(mesh):
    finer = Mesh(mesh.devices.reshape(2, 2, 2, 4, 4, 2), ("w", "v", "u", "y", "x", "c"))
    tm, tok = ("w", "v", "u", "y"), ("x", "c")
    placed = (
        P(tm, None, tok, None),
        P(tm, None, tok, None),
        P(None, tok, None),
        P(tm),
        P(tm, None, None),
        P(),
        P(tm, None),
        P(),
        P(),
    )
    return jax.shard_map(device_program, mesh=finer, in_specs=placed, out_specs=P(tm, None, tok, None), check_vma=False)
```

```python
import jax
import jax.numpy as jnp
from jax import lax
from jax.experimental import pallas as pl
from jax.experimental.pallas import tpu as pltpu
from jax.sharding import Mesh
from jax.sharding import PartitionSpec as P


HEADS = 16
HEAD_BATCH = 8
SWEEPS = 2
LANES = 128
LOG2E = 1.4426950408889634
SHARES = ("u", "y")
GROUPS = ("w", "v")
VMEM = pl.BlockSpec(memory_space=pltpu.VMEM)
SMEM = pl.BlockSpec(memory_space=pltpu.SMEM)


def shifted(value, axis, shift):
    size = lax.axis_size(axis)
    return lax.ppermute(value, axis, [(i, (i + shift) % size) for i in range(size)])


def spread(values, axis, sign=1):
    moved = []
    for k, value in enumerate(values, 1):
        moved.append(shifted(value, axis, sign * k))
    return moved


def call(body, outs, specs, *args, scratch=(), out_spec=VMEM):
    return pl.pallas_call(
        body,
        out_shape=outs,
        in_specs=specs,
        out_specs=jax.tree.map(lambda _: out_spec, outs),
        scratch_shapes=list(scratch),
        compiler_params=pltpu.CompilerParams(vmem_limit_bytes=16 * 2**20),
    )(*args)


def normed_rows(rows, shift, scale):
    center = jnp.mean(rows, axis=-1, keepdims=True)
    off = rows - center
    spread = jnp.mean(off * off, axis=-1, keepdims=True)
    normed = off / jnp.sqrt(spread + 1e-06)
    return (normed * (1.0 + scale) + shift).astype(jnp.bfloat16)


def modulation_row(where_ref, step_ref, view_ref, step, part):
    return step_ref[step, part : part + 1, :] + view_ref[where_ref[3 + step], part : part + 1, :]


def enter_body(where_ref, mine_ref, peer_ref, step_ref, view_ref, x_ref, *mod_refs):
    place = where_ref[0]
    steps = mine_ref.shape[0]
    for r in range(steps):
        step = lax.rem(place + r, steps)
        shift = modulation_row(where_ref, step_ref, view_ref, step, 0)
        scale = modulation_row(where_ref, step_ref, view_ref, step, 1)
        rows = jnp.concatenate([mine_ref[step], peer_ref[step]], axis=0)
        x_ref[step] = rows
        mod_refs[r][...] = normed_rows(rows, shift, scale)


def resume_body(
    where_ref, mine_start, peer_start, mine_before, peer_before, lower_ref, step_ref, view_ref, x_ref, *rest
):
    mod_refs, base_ref = rest[:-1], rest[-1]
    place = where_ref[0]
    steps = mine_before.shape[0]
    places, share, _ = lower_ref.shape
    for q in range(places):
        base_ref[q * share : (q + 1) * share, :] = lower_ref[q]
    start = jnp.concatenate([mine_start[...], peer_start[...]], axis=0)
    for r in range(steps):
        step = lax.rem(place + r, steps)
        before = jnp.concatenate([mine_before[step], peer_before[step]], axis=0)
        rows = start + (base_ref[...] + before)
        x_ref[step] = rows
        shift = modulation_row(where_ref, step_ref, view_ref, step, 0)
        scale = modulation_row(where_ref, step_ref, view_ref, step, 1)
        mod_refs[r][...] = normed_rows(rows, shift, scale)


def finish_body(
    where_ref, start_ref, mine_before, peer_before, mine_lower, peer_lower, out_ref, base_ref, rows_ref, sems
):
    core = where_ref[2]
    places, share, _ = mine_lower.shape
    half = places // 2
    sides = ((core, 0, mine_before, mine_lower), (1 - core, half, peer_before, peer_lower))
    copies = []
    for side, (view, low, before_ref, lower_ref) in enumerate(sides):
        for q in range(half):
            rows = slice(q * share, (q + 1) * share)
            base_ref[rows, :] = lower_ref[low + q]
        for step in range(before_ref.shape[0]):
            rows_ref[side, step] = start_ref[view] + (base_ref[...] + before_ref[step])
            copies.append(
                pltpu.make_async_copy(rows_ref.at[side, step], out_ref.at[step, view], sems.at[side, step])
            )
            copies[-1].start()
    for copy in copies:
        copy.wait()


def project_rows(rows, w_ref):
    return jnp.dot(rows, w_ref[...], preferred_element_type=jnp.float32).astype(jnp.bfloat16)


def first_body(a0, w_ref, qkv_ref):
    qkv_ref[...] = project_rows(a0[...], w_ref)


def attend(q_ref, kv_ref, mask_ref, outs, scores_ref, probs_ref):
    width = mask_ref.shape[1]
    part = outs[0].shape[0]
    size = width // HEADS
    batch = scores_ref.shape[0]
    tiles = [None] * (width // LANES)

    def window(h):
        first = h * size // LANES
        last = ((h + 1) * size - 1) // LANES
        return first, last, first * LANES, (last + 1) * LANES

    for start in range(0, HEADS, batch):
        heads = range(start, start + batch)
        shares = []
        for h in heads:
            _, _, low, high = window(h)
            q = q_ref[:, low:high] * mask_ref[h : h + 1, low:high]
            k = kv_ref[:, width + low : width + high]
            scores_ref[h - start] = lax.dot_general(
                q, k, (((1,), (1,)), ((), ())), preferred_element_type=jnp.float32
            )
        for h in heads:
            scores = scores_ref[h - start]
            top = jnp.max(scores, axis=-1, keepdims=True)
            powers = jnp.exp2((scores - top) * (LOG2E / size**0.5))
            shares.append(1.0 / jnp.sum(powers, axis=-1, keepdims=True))
            probs_ref[h - start] = powers.astype(jnp.bfloat16)
        for h in heads:
            first, last, low, high = window(h)
            v = kv_ref[:, 2 * width + low : 2 * width + high]
            out = jnp.dot(probs_ref[h - start], v, preferred_element_type=jnp.float32) * shares[h - start]
            for t in range(first, last + 1):
                piece = out[:, t * LANES - low : (t + 1) * LANES - low]
                if tiles[t] is not None:
                    lane = lax.broadcasted_iota(jnp.int32, piece.shape, 1) + t * LANES
                    piece = jnp.where(lane >= h * size, piece, tiles[t])
                tiles[t] = piece
                if (t + 1) * LANES <= (h + 1) * size:
                    tile = piece.astype(jnp.bfloat16)
                    for r, out_ref in enumerate(outs):
                        out_ref[:, t * LANES : (t + 1) * LANES] = tile[r * part : (r + 1) * part]


def stages(queries, keys):
    return [
        pltpu.VMEM((HEAD_BATCH, queries, keys), jnp.float32),
        pltpu.VMEM((HEAD_BATCH, queries, keys), jnp.bfloat16),
    ]


def others_body(
    first_ref, a1, a2, a3, w_ref, mask_ref, o1, o2, o3, qkv_ref, rows_ref, scores_ref, probs_ref
):
    part = a1.shape[0]
    for r, piece in enumerate((a1, a2, a3)):
        rows_ref[r * part : (r + 1) * part, :] = piece[...]
    qkv_ref[: 3 * part, :] = project_rows(rows_ref[...], w_ref)
    qkv_ref[3 * part :, :] = first_ref[...]
    attend(qkv_ref.at[: 3 * part], qkv_ref, mask_ref, (o1, o2, o3), scores_ref, probs_ref)


def own_body(first_ref, qkv_ref, mask_ref, o0, scores_ref, probs_ref):
    attend(first_ref, qkv_ref, mask_ref, (o0,), scores_ref, probs_ref)


def base_body(coef_ref, x_ref, mine_ref, peer_ref, base_ref):
    for step in range(x_ref.shape[0]):
        rows = x_ref[step]
        drawn = jnp.concatenate([mine_ref[step], peer_ref[step]], axis=0).astype(jnp.float32)
        base_ref[step] = (coef_ref[0, step] + coef_ref[1, step]) * rows + coef_ref[2, step] * drawn


def project_body(
    where_ref,
    coef_ref,
    a0,
    a1,
    a2,
    a3,
    w_ref,
    base_ref,
    step_ref,
    view_ref,
    mine_before,
    peer_before,
    total_ref,
    rows_ref,
    proj_ref,
):
    place = where_ref[0]
    pieces = (a0, a1, a2, a3)
    part = a0.shape[0]
    half = part // 2
    steps = len(pieces)
    for r in range(steps):
        rows = pl.ds(pl.multiple_of(lax.rem(place + r, steps) * part, part), part)
        rows_ref[rows, :] = pieces[r][...]
    proj_ref[...] = jnp.dot(rows_ref[...], w_ref[...], preferred_element_type=jnp.float32)
    running = jnp.zeros((part, proj_ref.shape[1]), jnp.float32)
    for step in range(steps):
        gate = modulation_row(where_ref, step_ref, view_ref, step, 2) * coef_ref[1, step]
        mine_before[step] = running[:half]
        peer_before[step] = running[half:]
        running = running + (base_ref[step] + gate * proj_ref[step * part : (step + 1) * part, :])
    places, share, _ = total_ref.shape
    for q in range(places):
        total_ref[q] = running[q * share : (q + 1) * share]


def coefficients(steps_index):
    unit = steps_index.astype(jnp.float32) / 1000.0
    beta = 0.1 + 19.9 * unit
    sigma = jnp.sqrt(1.0 - jnp.exp(-(0.1 * unit + 9.95 * unit * unit)))
    coef_state = 0.5 * beta * 0.004
    coef_eps = beta * 0.004 / sigma
    coef_noise = jnp.sqrt(beta * 0.004)
    return (coef_state, coef_eps, coef_noise)


def inside_body(held_ref, before_ref, all_ref):
    running = jnp.zeros(held_ref.shape[1:], held_ref.dtype)
    for q in range(held_ref.shape[0]):
        before_ref[q] = running
        running = running + held_ref[q]
    all_ref[...] = running


def below_body(where_ref, before_ref, *refs):
    passed, out_ref = refs[:-1], refs[-1]
    group = where_ref[1]
    below = jnp.zeros(before_ref.shape[1:], before_ref.dtype)
    for shift, ref in enumerate(passed, 1):
        below = below + jnp.where(shift <= group, ref[...], 0.0)
    for q in range(before_ref.shape[0]):
        out_ref[q] = before_ref[q] + below


def earlier_sum(where, shares, beside=None):
    held = lax.all_to_all(shares, SHARES, 0, 0, tiled=True)
    whole = jax.ShapeDtypeStruct(shares.shape, shares.dtype)
    before, total = call(inside_body, [whole, jax.ShapeDtypeStruct(shares.shape[1:], shares.dtype)], [VMEM], held)
    passed = spread([total] * (lax.axis_size(GROUPS) - 1), GROUPS)
    if beside is not None:
        passed[0], beside = lax.optimization_barrier((passed[0], shifted(beside, "c", 1)))
    sums = call(below_body, whole, [SMEM] + [VMEM] * (1 + len(passed)), where, before, *passed)
    return lax.all_to_all(sums, SHARES, 0, 0, tiled=True), beside


def device_program(states, noise, x_start, timesteps, step_mod, view_mod, view_ids, w_qkv, w_out):
    steps, views, part, width = states.shape
    place, group, core = (lax.axis_index(a) for a in ("x", GROUPS, "c"))
    other = 1 - core
    f32, bf16 = jnp.float32, jnp.bfloat16
    rows = 2 * part

    def own(a, axis):
        return lax.dynamic_index_in_dim(a, core, axis, keepdims=False)

    def given(a, axis):
        return lax.dynamic_index_in_dim(a, other, axis, keepdims=False)

    def shape(*dims, kind=f32):
        return jax.ShapeDtypeStruct(dims, kind)

    swapped = shifted(given(states, 1), "c", 1)
    states_mine = own(states, 1)
    where = jnp.concatenate([jnp.stack([place, group, core]).astype(jnp.int32), own(view_ids, 1)])
    coefs = jnp.stack(coefficients(timesteps))
    size = width // HEADS
    column = jnp.arange(width, dtype=jnp.int32)[None, :]
    head = jnp.arange(HEADS, dtype=jnp.int32)[:, None]
    mask = ((column >= head * size) & (column < (head + 1) * size)).astype(bf16)

    x_shape = shape(steps, rows, width)
    half = shape(steps, part, width)
    places = lax.axis_size(SHARES)
    piece = shape(rows, width, kind=bf16)
    x, *mods = call(
        enter_body,
        [x_shape] + [piece] * steps,
        [SMEM] + [VMEM] * 4,
        where,
        states_mine,
        swapped,
        step_mod,
        view_mod,
    )
    drawn, late, _ = lax.optimization_barrier((noise, x_start, mods[0]))
    start_mine, start_peer, noise_mine, noise_peer = lax.optimization_barrier(
        (own(late, 0), shifted(given(late, 0), "c", 1), own(drawn, 1), shifted(given(drawn, 1), "c", 1))
    )
    for sweep in range(SWEEPS):
        arrived = spread(mods[1:], "x")
        first = call(first_body, shape(rows, 3 * width, kind=bf16), [VMEM] * 2, mods[0], w_qkv)
        *attended, qkv = call(
            others_body,
            [piece] * (steps - 1) + [shape(steps * rows, 3 * width, kind=bf16)],
            [VMEM] * 6,
            first,
            *arrived,
            w_qkv,
            mask,
            scratch=[pltpu.VMEM(((steps - 1) * rows, width), bf16)] + stages((steps - 1) * rows, steps * rows),
        )
        back = spread(attended, "x", -1)
        kept = call(
            own_body, piece, [VMEM] * 3, first, qkv, mask, scratch=stages(rows, steps * rows)
        )
        base = call(base_body, x_shape, [SMEM] + [VMEM] * 3, coefs, x, noise_mine, noise_peer)
        mine_before, peer_before, total = call(
            project_body,
            [half, half, shape(places, rows // places, width)],
            [SMEM] * 2 + [VMEM] * 8,
            where,
            coefs,
            kept,
            *back,
            w_out,
            base,
            step_mod,
            view_mod,
            scratch=[pltpu.VMEM((steps * rows, width), bf16), pltpu.VMEM((steps * rows, width), f32)],
        )
        if sweep + 1 == SWEEPS:
            break
        lower, _ = earlier_sum(where, total)
        x, *mods = call(
            resume_body,
            [x_shape] + [piece] * steps,
            [SMEM] + [VMEM] * 7,
            where,
            start_mine,
            start_peer,
            mine_before,
            peer_before,
            lower,
            step_mod,
            view_mod,
            scratch=[pltpu.VMEM((rows, width), f32)],
        )
    lower, peer_before = earlier_sum(where, total, peer_before)
    return call(
        finish_body,
        shape(*states.shape),
        [SMEM] + [VMEM] * 5,
        where,
        x_start,
        mine_before,
        peer_before,
        lower,
        shifted(lower, "c", 1),
        scratch=[
            pltpu.VMEM((part, width), f32),
            pltpu.VMEM((views, steps, part, width), f32),
            pltpu.SemaphoreType.DMA((views, steps)),
        ],
        out_spec=pl.BlockSpec(memory_space=pl.ANY),
    )


def solution(mesh):
    finer = Mesh(mesh.devices.reshape(2, 2, 2, 4, 4, 2), ("w", "v", "u", "y", "x", "c"))
    tm, tok = ("w", "v", "u", "y"), ("x", "c")
    placed = (
        P(tm, None, tok, None),
        P(tm, None, tok, None),
        P(None, tok, None),
        P(tm),
        P(tm, None, None),
        P(),
        P(tm, None),
        P(),
        P(),
    )
    return jax.shard_map(device_program, mesh=finer, in_specs=placed, out_specs=P(tm, None, tok, None), check_vma=False)
```
